32 devices in a mesh: group: 8 (over z, y), tok: 4 (over x, core).
Axes of the slice: x: 2, y: 2, z: 4, core: 2. Of those that a mesh axis runs over, the one named last changes fastest.
Arguments:
- tokens: bfloat16 [16384, 2048], P(('group', 'tok')), may hold values from -94 to 94
- learning_rates: float32 [2, 16384], P(None, 'group'), may hold values from 0.1 to 1
- channel_gains: float32 [2, 5, 2048], P(None, None, 'tok'), may hold values from 0.3 to 3
- fast_init: float32 [2, 3, 16, 128, 128], P(None, None, 'tok'), may hold values from -0.5 to 0.5
- step_size: float32 [2, 16], P(None, 'tok'), may hold values from 0.05 to 1
- update_table: int32 [2, 8], replicated, may hold values 0 or 1
Outputs:
- mixed: bfloat16 [16384, 2048], P(('group', 'tok'))
The draws below stay inside these ranges and needn't reach their ends.
All inputs are finite; a program needn't handle non-finite values.
Results may differ from the reference program's by a relative error of at most 0.033.
Values may be sent and summed in bfloat16 or wider, within the bound.
A program may use at most 64 MiB of HBM per device.

```python
import math
import jax
import jax.numpy as jnp
from jax import lax

D = 2048
HEADS = 16
HEAD = 128
LAYERS = 2
NS_STEPS = 5
GROUPS = 8
GROUP_TOK = 2048
TOKENS = 16384


def draw_tokens(key, part):
    key_base = jax.random.fold_in(key, 11)
    key_jitter = jax.random.fold_in(key, 12)
    normal_draw = jnp.clip(jax.random.normal(key_base, (TOKENS, D), jnp.float32), -6.0, 6.0)
    channel_ramp = 3.0 ** (jnp.arange(D, dtype=jnp.float32) / D)
    jitter = jax.random.uniform(key_jitter, (D,), jnp.float32, 0.7, 1.3)
    values = normal_draw * (channel_ramp * jitter)[None, :]
    return values.astype(jnp.bfloat16)


def plant(array, own_key, least, largest):
    extent = array.shape
    index_at = [jax.random.randint(jax.random.fold_in(own_key, axis), (), 0, extent[axis]) for axis in range(len(extent))]
    array = array.at[tuple(index_at)].set(least)
    longest = extent.index(max(extent))
    index_at[longest] = (index_at[longest] + 1) % extent[longest]
    return array.at[tuple(index_at)].set(largest)


def steps_of(rng, dims, cuts, least, largest):
    def one(dim, shards_of):
        heights = jax.random.uniform(jax.random.fold_in(jax.random.fold_in(rng, 6), dim), (shards_of,), jnp.float32, least / len(cuts), largest / len(cuts))
        return jnp.repeat(jnp.exp(heights), dims[dim] // shards_of).reshape((-1,) + (1,) * (len(dims) - dim - 1))

    loudness = one(*cuts[0])
    for cut in cuts[1:]:
        loudness = loudness * one(*cut)
    return loudness


def normal_values(own_key, shape, deviation, most, pieces=(), held_as=jnp.bfloat16):
    level = steps_of(own_key, shape, pieces, -0.22, 0.18) if pieces else 1.0
    result = jax.random.normal(own_key, shape, jnp.float32) * deviation * level
    return jnp.minimum(jnp.maximum(result, -most), most).astype(held_as)


def setup_inputs(seed: int = 0) -> dict:
    splits = jax.random.split(jax.random.key(seed), 7)
    return {
        "tokens": draw_tokens(jax.random.fold_in(splits[6], 71), 0),
        "learning_rates": jnp.clip(jnp.exp(math.log(1.0) - 2.3025851 * jax.random.uniform(splits[1], (LAYERS, TOKENS), jnp.float32) ** steps_of(splits[1], (LAYERS, TOKENS), ((1, 8),), -0.2, 0.2)), 0.1, 1.0),
        "channel_gains": jnp.clip(jnp.exp(math.log(3.0) - 2.3025851 * jax.random.uniform(splits[2], (LAYERS, 5, D), jnp.float32) ** steps_of(splits[2], (LAYERS, 5, D), ((2, 4),), -0.2, 0.2)), 0.3, 3.0),
        "fast_init": normal_values(splits[3], (LAYERS, 3, HEADS, HEAD, HEAD), HEAD ** -0.5, 0.5, ((2, 4),), jnp.float32),
        "step_size": jnp.clip(jnp.exp(math.log(1.0) - 2.9957323 * jax.random.uniform(splits[4], (LAYERS, HEADS), jnp.float32) ** steps_of(splits[4], (LAYERS, HEADS), ((1, 4),), -0.2, 0.2)), 0.05, 1.0),
        "update_table": plant((jax.random.randint(splits[5], (LAYERS, GROUPS), 0, 4) < 3).astype(jnp.int32), jax.random.fold_in(splits[5], 1), 0, 1),
    }


MUON_A = 3.4445
MUON_B = -4.775
MUON_C = 2.0315
EPSILON = 1e-06

def orthogonalize(gradient):
    scaling = lax.rsqrt(lax.optimization_barrier(jnp.sum(gradient * gradient, axis=(-2, -1), keepdims=True)) + EPSILON)
    current = gradient * scaling
    for repeat in range(NS_STEPS):
        square = jnp.einsum('...ij,...kj->...ik', current, current, precision=lax.Precision.HIGHEST)
        polynom = MUON_B * square + MUON_C * jnp.einsum('...ij,...jk->...ik', square, square, precision=lax.Precision.HIGHEST)
        current = MUON_A * current + jnp.einsum('...ij,...jk->...ik', polynom, current, precision=lax.Precision.HIGHEST)
    return current

def layer_group(stream, entering, gain_rows, rates_row, steps_row, update_flag, inverse):
    row_count, channel_count = stream.shape
    heads_n = entering.shape[1]
    head_dim = entering.shape[2]
    normed = stream.astype(jnp.float32) * inverse[:, None] * gain_rows[0]
    queries = (normed * gain_rows[1]).astype(jnp.bfloat16).reshape(row_count, heads_n, head_dim).astype(jnp.float32)
    keys_in = (normed * gain_rows[2]).astype(jnp.bfloat16).reshape(row_count, heads_n, head_dim).astype(jnp.float32)
    values_in = (normed * gain_rows[3]).astype(jnp.bfloat16).reshape(row_count, heads_n, head_dim).astype(jnp.float32)
    rounded = entering.astype(jnp.bfloat16).astype(jnp.float32)
    gate_q = jnp.einsum('thi,hij->thj', queries, rounded[0])
    up_q = jnp.einsum('thi,hij->thj', queries, rounded[1])
    hidden_q = (jax.nn.silu(gate_q) * up_q).astype(jnp.bfloat16).astype(jnp.float32)
    output = jnp.einsum('thj,hjk->thk', hidden_q, rounded[2]).reshape(row_count, channel_count)
    mixed_rows = (stream.astype(jnp.float32) + gain_rows[4] * output).astype(jnp.bfloat16)
    gate_k = jnp.einsum('thi,hij->thj', keys_in, rounded[0])
    up_k = jnp.einsum('thi,hij->thj', keys_in, rounded[1])
    sigmoid_k = jax.nn.sigmoid(gate_k)
    active_k = gate_k * sigmoid_k
    hidden_k = (active_k * up_k).astype(jnp.bfloat16).astype(jnp.float32)
    targets = (rates_row[:, None, None] * values_in).astype(jnp.bfloat16).astype(jnp.float32)
    back_hidden = jnp.einsum('thk,hjk->thj', targets, rounded[2])
    back_up = (back_hidden * active_k).astype(jnp.bfloat16).astype(jnp.float32)
    back_gate = (back_hidden * up_k * sigmoid_k * (1.0 + gate_k * (1.0 - sigmoid_k))).astype(jnp.bfloat16).astype(jnp.float32)
    grad_gate = jnp.einsum('thi,thj->hij', keys_in, back_gate)
    grad_up = jnp.einsum('thi,thj->hij', keys_in, back_up)
    grad_down = jnp.einsum('thj,thk->hjk', hidden_k, targets)
    direction = orthogonalize(jnp.stack([grad_gate, grad_up, grad_down]))
    moved_state = entering + (update_flag * steps_row)[None, :, None, None] * direction
    norm_before = jnp.sqrt(lax.optimization_barrier(jnp.sum(entering * entering, axis=2, keepdims=True)) + EPSILON)
    norm_after = jnp.sqrt(lax.optimization_barrier(jnp.sum(moved_state * moved_state, axis=2, keepdims=True)) + EPSILON)
    return (mixed_rows, moved_state * (norm_before / norm_after))

def reference(tokens, learning_rates, channel_gains, fast_init, step_size, update_table):
    stream = tokens.reshape(GROUPS, GROUP_TOK, D)
    for layer_index in range(LAYERS):

        def advance(weights, inputs):
            block_rows, rates_row, update_flag = inputs
            widened = block_rows.astype(jnp.float32)
            inverse = lax.rsqrt(lax.optimization_barrier(jnp.sum(widened * widened, axis=1)) / D + EPSILON)
            mixed_rows, updated = layer_group(block_rows, weights, channel_gains[layer_index], rates_row, step_size[layer_index], update_flag, inverse)
            return (updated, mixed_rows)
        rates_blocks = learning_rates[layer_index].reshape(GROUPS, GROUP_TOK)
        flags = update_table[layer_index].astype(jnp.float32)
        last_state, stream = lax.scan(advance, fast_init[layer_index], (stream, rates_blocks, flags))
    return stream.reshape(TOKENS, D)
```

```python
import functools

import jax
import jax.numpy as jnp
from jax import lax
from jax.experimental import pallas as pl
from jax.experimental.pallas import tpu as pltpu
from jax.sharding import PartitionSpec as P

NS_STEPS = 5


MUON_A = 3.4445
MUON_B = -4.775
MUON_C = 2.0315
EPSILON = 1e-06


def passed_along(value, axis, by):
    size = lax.axis_size(axis)
    pairs = [(i, i + by) for i in range(size) if 0 <= i + by < size]
    return lax.ppermute(value, axis, pairs)


def orthogonalize(gradient):
    scaling = lax.rsqrt(jnp.sum(gradient * gradient, axis=(-2, -1), keepdims=True) + EPSILON)
    current = gradient * scaling
    for repeat in range(NS_STEPS):
        square = jnp.einsum("...ij,...kj->...ik", current, current, precision=lax.Precision.HIGHEST)
        polynom = MUON_B * square + MUON_C * jnp.einsum(
            "...ij,...jk->...ik", square, square, precision=lax.Precision.HIGHEST
        )
        current = MUON_A * current + jnp.einsum(
            "...ij,...jk->...ik", polynom, current, precision=lax.Precision.HIGHEST
        )
    return current


def layer_group(stream, entering, gain_rows, rates_row, steps_row, update_flag, inverse):
    row_count, channel_count = stream.shape
    heads_n = entering.shape[1]
    head_dim = entering.shape[2]
    normed = stream.astype(jnp.float32) * inverse[:, None] * gain_rows[0]
    queries = (normed * gain_rows[1]).astype(jnp.bfloat16).reshape(row_count, heads_n, head_dim)
    keys_in = (normed * gain_rows[2]).astype(jnp.bfloat16).reshape(row_count, heads_n, head_dim)
    values_in = (normed * gain_rows[3]).astype(jnp.bfloat16).reshape(row_count, heads_n, head_dim)
    rounded = entering.astype(jnp.bfloat16)
    gate_q = jnp.einsum("thi,hij->thj", queries, rounded[0], preferred_element_type=jnp.float32)
    up_q = jnp.einsum("thi,hij->thj", queries, rounded[1], preferred_element_type=jnp.float32)
    hidden_q = (jax.nn.silu(gate_q) * up_q).astype(jnp.bfloat16)
    output = jnp.einsum(
        "thj,hjk->thk", hidden_q, rounded[2], preferred_element_type=jnp.float32
    ).reshape(row_count, channel_count)
    mixed_rows = (stream.astype(jnp.float32) + gain_rows[4] * output).astype(jnp.bfloat16)
    gate_k = jnp.einsum("thi,hij->thj", keys_in, rounded[0], preferred_element_type=jnp.float32)
    up_k = jnp.einsum("thi,hij->thj", keys_in, rounded[1], preferred_element_type=jnp.float32)
    sigmoid_k = jax.nn.sigmoid(gate_k)
    active_k = gate_k * sigmoid_k
    hidden_k = (active_k * up_k).astype(jnp.bfloat16)
    targets = (rates_row[:, None, None] * values_in.astype(jnp.float32)).astype(jnp.bfloat16)
    back_hidden = jnp.einsum(
        "thk,hjk->thj", targets, rounded[2], preferred_element_type=jnp.float32
    )
    back_up = (back_hidden * active_k).astype(jnp.bfloat16)
    back_gate = (back_hidden * up_k * sigmoid_k * (1.0 + gate_k * (1.0 - sigmoid_k))).astype(
        jnp.bfloat16
    )
    grad_gate = jnp.einsum("thi,thj->hij", keys_in, back_gate, preferred_element_type=jnp.float32)
    grad_up = jnp.einsum("thi,thj->hij", keys_in, back_up, preferred_element_type=jnp.float32)
    grad_down = jnp.einsum("thj,thk->hjk", hidden_k, targets, preferred_element_type=jnp.float32)
    direction = orthogonalize(jnp.stack([grad_gate, grad_up, grad_down]))
    moved_state = entering + (update_flag * steps_row)[None, :, None, None] * direction
    norm_before = jnp.sqrt(jnp.sum(entering * entering, axis=2, keepdims=True) + EPSILON)
    norm_after = jnp.sqrt(jnp.sum(moved_state * moved_state, axis=2, keepdims=True) + EPSILON)
    return (mixed_rows, moved_state * (norm_before / norm_after))


def pass_on(outgoing):
    return passed_along(outgoing, "group", 1)


def body(tokens, learning_rates, channel_gains, fast_init, step_size, update_table):
    start_stream = lax.all_to_all(tokens, "tok", split_axis=1, concat_axis=0, tiled=True)
    group_count = lax.axis_size("group")
    group_index = lax.axis_index("group")
    width_all = start_stream.shape[1] * lax.axis_size("tok")
    layer_count = fast_init.shape[0]
    zero_state = jnp.zeros(fast_init.shape[1:], jnp.float32)

    def tick_work(stream, outgoing, layer_now, active, inverse):
        received = pass_on(outgoing)
        initial = lax.dynamic_index_in_dim(fast_init, layer_now, 0, keepdims=False)
        entering = jnp.where(group_index == 0, initial, received)
        gain_rows = lax.dynamic_index_in_dim(channel_gains, layer_now, 0, keepdims=False)
        rates_row = lax.dynamic_index_in_dim(learning_rates, layer_now, 0, keepdims=False)
        steps_row = lax.dynamic_index_in_dim(step_size, layer_now, 0, keepdims=False)
        table_cell = lax.dynamic_slice(
            update_table, (jnp.asarray(layer_now, jnp.int32), group_index), (1, 1)
        )
        update_flag = table_cell[0, 0].astype(jnp.float32)

        def working(operands):
            return layer_group(
                operands[0], operands[1], gain_rows, rates_row, steps_row, update_flag, inverse
            )

        def resting(operands):
            return (operands[0], operands[2])

        return lax.cond(active, working, resting, (stream, entering, outgoing))

    def one_tick(tick_index, loop_state):
        stream, outgoing = loop_state
        layer_raw = tick_index - group_index
        active = (layer_raw >= 0) & (layer_raw < layer_count)
        layer_now = jnp.clip(layer_raw, 0, layer_count - 1)
        widened = stream.astype(jnp.float32)
        totals = lax.psum(jnp.sum(widened * widened, axis=1), "tok")
        inverse = lax.rsqrt(totals / width_all + EPSILON)
        return tick_work(stream, outgoing, layer_now, active, inverse)

    final_stream, last_state = lax.fori_loop(
        0, layer_count + group_count - 1, one_tick, (start_stream, zero_state)
    )
    return lax.all_to_all(final_stream, "tok", split_axis=0, concat_axis=1, tiled=True)


MESH = pl.DeviceIdType.MESH
F32 = jnp.float32
BF16 = jnp.bfloat16
NN = (((1,), (0,)), ((), ()))
NT = (((1,), (1,)), ((), ()))
TN = (((0,), (0,)), ((), ()))


def dot(a, b, dims=NN):
    return lax.dot_general(a, b, dims, preferred_element_type=F32)


def halves(value):
    high = value.astype(BF16)
    return high, (value - high.astype(F32)).astype(BF16)


def product(a, b):
    a_high, a_low = halves(a)
    b_high, b_low = halves(b)
    left = jnp.concatenate([a_high, a_low], axis=1)
    above = jnp.concatenate([b_high, b_low], axis=1)
    below = jnp.concatenate([b_high, jnp.zeros_like(b_low)], axis=1)
    both = dot(left, jnp.concatenate([above, below], axis=0))
    return both[:, : b.shape[1]] + both[:, b.shape[1] :]


def gram(a):
    high, low = halves(a)
    left = jnp.concatenate([high, low], axis=1)
    above = jnp.concatenate([high, high], axis=1)
    below = jnp.concatenate([low, jnp.zeros_like(low)], axis=1)
    both = dot(left, jnp.concatenate([above, below], axis=0), NT)
    return both[:, : a.shape[0]] + both[:, a.shape[0] :]


def sigmoid(value):
    return 0.5 * jnp.tanh(0.5 * value) + 0.5


def newton_schulz(values):
    squares = [gram(v) for v in values]
    polynoms = [MUON_B * q + MUON_C * product(q, q) for q in squares]
    return tuple(MUON_A * v + product(p, v) for p, v in zip(polynoms, values))


def wave_kernel(
    sizes,
    steps,
    table,
    tokens,
    rates,
    gains,
    initial,
    out,
    xin,
    xout,
    weights,
    leaving,
    totals,
    squares,
    partial,
    partials,
    stack,
    grad_gu,
    grad_d,
    t_send,
    t_recv,
    s_send,
    s_recv,
    p_send,
    p_recv,
    w_send,
    w_recv,
    o_send,
    o_recv,
):
    groups, toks, layers, owned, rows, width, tile = sizes
    group_tok = rows * toks
    g = lax.axis_index("group")
    t = lax.axis_index("tok")
    last = groups - 1

    def remote(source, target, send, recv, to_g, to_t):
        return pltpu.make_async_remote_copy(
            src_ref=source,
            dst_ref=target,
            send_sem=send,
            recv_sem=recv,
            device_id=(to_g, to_t),
            device_id_type=MESH,
        )

    def arrived(target, recv):
        pltpu.make_async_copy(target, target, recv).wait()

    def lane(index, size):
        return pl.ds(pl.multiple_of(index * size, size), size)

    barrier = pltpu.get_barrier_semaphore()

    def greet(to_g, to_t):
        pl.semaphore_signal(barrier, inc=1, device_id=(to_g, to_t), device_id_type=MESH)

    for step in range(1, toks):
        greet(g, lax.rem(t + step, toks))

    greet(lax.rem(g + 1, groups), t)
    greet(lax.rem(g + last, groups), t)
    pl.semaphore_wait(barrier, toks + 1)

    def peer(step):
        return lax.rem(t + step, toks)

    def hand_out(j):
        for step in [2, 3, 1, 0] if toks == 4 else range(toks):
            to_t = peer(step)
            source = tokens.at[:, lane(to_t * owned + j, width)]
            target = xin.at[0, j, lane(t, rows)]
            if step == 0:
                pltpu.make_async_copy(source, target, t_recv.at[j, t]).start()
            else:
                remote(source, target, t_send.at[j, step], t_recv.at[j, t], g, to_t).start()

    hand_out(0)
    ones_rows = jnp.ones((16, width), BF16)

    def sums_of(values):
        wide = values.astype(F32)
        return dot(ones_rows, (wide * wide).astype(BF16), NT)[0:1]

    totals[...] = jnp.zeros_like(totals)

    @pl.loop(0, owned * toks)
    def _(h):
        totals[...] += sums_of(tokens[:, lane(h, width)])

    squares[t] = totals[...]
    for step in range(1, toks):
        remote(totals, squares.at[t], s_send.at[step], s_recv.at[t], g, peer(step)).start()

    @pl.loop(1, owned)
    def _(j):
        hand_out(j)

    @pl.when(g == 0)
    def _():
        for l in range(layers):
            @pl.loop(0, owned)
            def _(j):
                for which in range(3):
                    weights[l, j, :, which * width : (which + 1) * width] = initial[
                        l, which, j
                    ].astype(BF16)

    pick_row = lax.broadcasted_iota(jnp.int32, (16, 2 * width), 0)
    pick_lane = lax.broadcasted_iota(jnp.int32, (16, 2 * width), 1)
    spread = jnp.where(pick_row // 2 == pick_lane // width, 1.0, 0.0).astype(BF16)

    def scale_rows(l, at, sums):
        size = sums.shape[1]
        inverse = lax.rsqrt(sums / (owned * toks * width) + EPSILON)
        rate = rates[l : l + 1, at]
        inverse_high = inverse.astype(BF16).astype(F32)
        rate_high = rate.astype(BF16).astype(F32)
        at_row = lax.broadcasted_iota(jnp.int32, (16, size), 0)
        fill = jnp.where(at_row == 0, inverse_high, 0.0)
        fill = jnp.where(at_row == 1, inverse - inverse_high, fill)
        fill = jnp.where(at_row == 2, rate_high, fill)
        stack[:, at] = jnp.where(at_row == 3, rate - rate_high, fill).astype(BF16)

    def gains_of(l, j):
        rows_of = gains[l, :, lane(j, width)]
        norm = rows_of[0:1]
        return norm * rows_of[1:2], norm * rows_of[2:3], norm * rows_of[3:4], rows_of[4:5]

    def query(l, j):
        query_gain, _, _, out_gain = gains_of(l, j)
        size = min(tile, group_tok)

        @pl.loop(0, group_tok // size)
        def _(i):
            here = lane(i, size)
            stream = xin[l, j, here, :].astype(F32)
            normed = stream * dot(stack[:, here], spread[:, :width], TN)
            queries = (normed * query_gain).astype(BF16)
            both = dot(queries, weights[l, j, :, : 2 * width])
            gate = both[:, :width]
            hidden = (gate * sigmoid(gate) * both[:, width:]).astype(BF16)
            mixed = (stream + out_gain * dot(hidden, weights[l, j, :, 2 * width :])).astype(BF16)
            if l < layers - 1:
                xin[l + 1, j, here, :] = mixed
                partial[l, :, here] += sums_of(mixed)
            else:
                xout[j, here, :] = mixed

        if l == layers - 1:
            for step in [2, 3, 1, 0] if toks == 4 else range(toks):
                to_t = peer(step)
                source = xout.at[j, lane(to_t, rows)]
                target = out.at[:, lane(t * owned + j, width)]
                if step == 0:
                    pltpu.make_async_copy(source, target, o_recv).start()
                else:
                    remote(source, target, o_send.at[j, step], o_recv, g, to_t).start()

    def learn(l, j):
        _, key_gain, value_gain, _ = gains_of(l, j)
        size = min(tile, group_tok)
        grad_gu[...] = jnp.zeros_like(grad_gu)
        grad_d[...] = jnp.zeros_like(grad_d)

        @pl.loop(0, group_tok // size)
        def _(i):
            here = lane(i, size)
            scale = dot(stack[:, here], spread, TN)
            normed = xin[l, j, here, :].astype(F32) * scale[:, :width]
            keys = (normed * key_gain).astype(BF16)
            targets = (normed * value_gain * scale[:, width:]).astype(BF16)
            both = dot(keys, weights[l, j, :, : 2 * width])
            back = dot(targets, weights[l, j, :, 2 * width :], NT)
            gate = both[:, :width]
            up = both[:, width:]
            sig = sigmoid(gate)
            act = gate * sig
            hidden = (act * up).astype(BF16)
            back_up = (back * act).astype(BF16)
            back_gate = (back * up * (sig + act * (1.0 - sig))).astype(BF16)
            backs = jnp.concatenate([back_gate, back_up], axis=1)
            grad_gu[...] += dot(keys, backs, TN)
            grad_d[...] += dot(hidden, targets, TN)

    def chain(l, j):
        @pl.when(g > 0)
        def _():
            arrived(weights.at[l, j], w_recv.at[l, j])

        chain_go(l, j)

    def chain_go(l, j):
        @pl.when(g < last)
        def _():
            learn(l, j)
            grads = (grad_gu[:, :width], grad_gu[:, width:], grad_d[...])
            moves = tuple(
                v * lax.rsqrt(jnp.sum(v * v, axis=(0, 1), keepdims=True) + EPSILON) for v in grads
            )
            for _ in range(NS_STEPS):
                moves = newton_schulz(moves)
            step = steps[l, j] * table[l, g].astype(F32)
            for which in range(3):
                at = slice(which * width, (which + 1) * width)
                entering = weights[l, j, :, at].astype(F32)
                moved = entering + step * moves[which]
                before = jnp.sum(entering * entering, axis=0, keepdims=True) + EPSILON
                after = jnp.sum(moved * moved, axis=0, keepdims=True) + EPSILON
                leaving[l, j, :, at] = (moved * (jnp.sqrt(before) * lax.rsqrt(after))).astype(BF16)
            remote(
                leaving.at[l, j], weights.at[l, j], w_send.at[l, j], w_recv.at[l, j], g + 1, t
            ).start()

    def await_tokens(j):
        for k in range(toks):
            arrived(xin.at[0, j, pl.ds(k * rows, rows)], t_recv.at[j, k])

    for step in range(1, toks):
        arrived(squares.at[peer(step)], s_recv.at[peer(step)])
    for k in range(toks):
        scale_rows(0, slice(k * rows, (k + 1) * rows), squares[k])

    for l in range(layers):
        if l > 0:
            arrived_sums = partial[l - 1]
            for step in range(1, toks):
                arrived(partials.at[l - 1, peer(step)], p_recv.at[l - 1, peer(step)])
                arrived_sums += partials[l - 1, peer(step)]
            scale_rows(l, slice(0, group_tok), arrived_sums)
        if l < layers - 1:
            partial[l] = jnp.zeros((1, group_tok), F32)

            @pl.loop(0, owned - 1)
            def _(j):
                if l == 0:
                    await_tokens(j)
                chain(l, j)
                query(l, j)

            if l == 0:
                await_tokens(owned - 1)

            @pl.when(g > 0)
            def _():
                arrived(weights.at[l, owned - 1], w_recv.at[l, owned - 1])

            query(l, owned - 1)
            for step in range(1, toks):
                remote(
                    partial.at[l],
                    partials.at[l, t],
                    p_send.at[l, step],
                    p_recv.at[l, t],
                    g,
                    peer(step),
                ).start()
            chain_go(l, owned - 1)
        else:
            @pl.loop(0, owned)
            def _(j):
                chain(l, j)

                @pl.when(g == last)
                def _():
                    query(l, j)

            @pl.when(g < last)
            def _():
                @pl.loop(0, owned)
                def _(j):
                    query(l, j)

    arrived(out, o_recv)

    @pl.loop(0, owned)
    def _(j):
        for step in range(1, toks):
            source = tokens.at[:, lane(peer(step) * owned + j, width)]
            pltpu.make_async_copy(source, source, t_send.at[j, step]).wait()
            block = xout.at[j, lane(peer(step), rows)]
            pltpu.make_async_copy(block, block, o_send.at[j, step]).wait()

        @pl.when(g < last)
        def _():
            for l in range(layers):
                arrived(leaving.at[l, j], w_send.at[l, j])

    for step in range(1, toks):
        arrived(totals, s_send.at[step])
        for l in range(layers - 1):
            arrived(partial.at[l], p_send.at[l, step])


def wave_body(tokens, learning_rates, channel_gains, fast_init, step_size, update_table):
    groups, toks = lax.axis_size("group"), lax.axis_size("tok")
    layers, _, owned, width, _ = fast_init.shape
    rows, channels = tokens.shape
    group_tok = rows * toks
    sizes = (groups, toks, layers, owned, rows, width, TILE)
    vmem = pl.BlockSpec(memory_space=pltpu.VMEM)
    smem = pl.BlockSpec(memory_space=pltpu.SMEM)
    anywhere = pl.BlockSpec(memory_space=pl.ANY)
    dma = pltpu.SemaphoreType.DMA
    return pl.pallas_call(
        functools.partial(wave_kernel, sizes),
        out_shape=jax.ShapeDtypeStruct((rows, channels), BF16),
        in_specs=[smem, smem, vmem, vmem, vmem, vmem],
        out_specs=anywhere,
        scratch_shapes=[
            pltpu.VMEM((layers, owned, group_tok, width), BF16),
            pltpu.VMEM((owned, group_tok, width), BF16),
            pltpu.VMEM((layers, owned, width, 3 * width), BF16),
            pltpu.VMEM((layers, owned, width, 3 * width), BF16),
            pltpu.VMEM((1, rows), F32),
            pltpu.VMEM((toks, 1, rows), F32),
            pltpu.VMEM((layers - 1, 1, group_tok), F32),
            pltpu.VMEM((layers - 1, toks, 1, group_tok), F32),
            pltpu.VMEM((16, group_tok), BF16),
            pltpu.VMEM((width, 2 * width), F32),
            pltpu.VMEM((width, width), F32),
            dma((owned, toks)),
            dma((owned, toks)),
            dma((toks,)),
            dma((toks,)),
            dma((layers - 1, toks)),
            dma((layers - 1, toks)),
            dma((layers, owned)),
            dma((layers, owned)),
            dma((owned, toks)),
            dma,
        ],
        compiler_params=pltpu.CompilerParams(
            collective_id=0, has_side_effects=True, vmem_limit_bytes=48 * 1024 * 1024
        ),
    )(step_size, update_table, tokens, learning_rates, channel_gains, fast_init)


TILE = 1024


def plan(mesh, tokens, fast_init):
    groups, toks = mesh.shape["group"], mesh.shape["tok"]
    layers, _, heads, width, _ = fast_init.shape
    rows = tokens.shape[0] // (groups * toks)
    fits = groups > 1 and toks > 1 and layers > 1 and heads % toks == 0
    fits = fits and rows * toks % TILE == 0 and rows % 128 == 0 and width % 128 == 0
    return wave_body if fits and tokens.shape[0] * tokens.shape[1] <= 64 * 1024 * 1024 else body


def solution(mesh):
    in_specs = (
        P(("group", "tok"), None),
        P(None, "group"),
        P(None, None, "tok"),
        P(None, None, "tok", None, None),
        P(None, "tok"),
        P(),
    )
    out_specs = P(("group", "tok"), None)
    def run(*args):
        chosen = plan(mesh, args[0], args[3])
        return jax.shard_map(
            chosen, mesh=mesh, in_specs=in_specs, out_specs=out_specs, check_vma=False
        )(*args)

    return run
```

```python
import functools

import jax
import jax.numpy as jnp
from jax import lax
from jax.experimental import pallas as pl
from jax.experimental.pallas import tpu as pltpu
from jax.sharding import PartitionSpec as P

NS_STEPS = 5


MUON_A = 3.4445
MUON_B = -4.775
MUON_C = 2.0315
EPSILON = 1e-06


def passed_along(value, axis, by):
    size = lax.axis_size(axis)
    pairs = [(i, i + by) for i in range(size) if 0 <= i + by < size]
    return lax.ppermute(value, axis, pairs)


def orthogonalize(gradient):
    scaling = lax.rsqrt(jnp.sum(gradient * gradient, axis=(-2, -1), keepdims=True) + EPSILON)
    current = gradient * scaling
    for repeat in range(NS_STEPS):
        square = jnp.einsum("...ij,...kj->...ik", current, current, precision=lax.Precision.HIGHEST)
        polynom = MUON_B * square + MUON_C * jnp.einsum(
            "...ij,...jk->...ik", square, square, precision=lax.Precision.HIGHEST
        )
        current = MUON_A * current + jnp.einsum(
            "...ij,...jk->...ik", polynom, current, precision=lax.Precision.HIGHEST
        )
    return current


def layer_group(stream, entering, gain_rows, rates_row, steps_row, update_flag, inverse):
    row_count, channel_count = stream.shape
    heads_n = entering.shape[1]
    head_dim = entering.shape[2]
    normed = stream.astype(jnp.float32) * inverse[:, None] * gain_rows[0]
    queries = (normed * gain_rows[1]).astype(jnp.bfloat16).reshape(row_count, heads_n, head_dim)
    keys_in = (normed * gain_rows[2]).astype(jnp.bfloat16).reshape(row_count, heads_n, head_dim)
    values_in = (normed * gain_rows[3]).astype(jnp.bfloat16).reshape(row_count, heads_n, head_dim)
    rounded = entering.astype(jnp.bfloat16)
    gate_q = jnp.einsum("thi,hij->thj", queries, rounded[0], preferred_element_type=jnp.float32)
    up_q = jnp.einsum("thi,hij->thj", queries, rounded[1], preferred_element_type=jnp.float32)
    hidden_q = (jax.nn.silu(gate_q) * up_q).astype(jnp.bfloat16)
    output = jnp.einsum(
        "thj,hjk->thk", hidden_q, rounded[2], preferred_element_type=jnp.float32
    ).reshape(row_count, channel_count)
    mixed_rows = (stream.astype(jnp.float32) + gain_rows[4] * output).astype(jnp.bfloat16)
    gate_k = jnp.einsum("thi,hij->thj", keys_in, rounded[0], preferred_element_type=jnp.float32)
    up_k = jnp.einsum("thi,hij->thj", keys_in, rounded[1], preferred_element_type=jnp.float32)
    sigmoid_k = jax.nn.sigmoid(gate_k)
    active_k = gate_k * sigmoid_k
    hidden_k = (active_k * up_k).astype(jnp.bfloat16)
    targets = (rates_row[:, None, None] * values_in.astype(jnp.float32)).astype(jnp.bfloat16)
    back_hidden = jnp.einsum(
        "thk,hjk->thj", targets, rounded[2], preferred_element_type=jnp.float32
    )
    back_up = (back_hidden * active_k).astype(jnp.bfloat16)
    back_gate = (back_hidden * up_k * sigmoid_k * (1.0 + gate_k * (1.0 - sigmoid_k))).astype(
        jnp.bfloat16
    )
    grad_gate = jnp.einsum("thi,thj->hij", keys_in, back_gate, preferred_element_type=jnp.float32)
    grad_up = jnp.einsum("thi,thj->hij", keys_in, back_up, preferred_element_type=jnp.float32)
    grad_down = jnp.einsum("thj,thk->hjk", hidden_k, targets, preferred_element_type=jnp.float32)
    direction = orthogonalize(jnp.stack([grad_gate, grad_up, grad_down]))
    moved_state = entering + (update_flag * steps_row)[None, :, None, None] * direction
    norm_before = jnp.sqrt(jnp.sum(entering * entering, axis=2, keepdims=True) + EPSILON)
    norm_after = jnp.sqrt(jnp.sum(moved_state * moved_state, axis=2, keepdims=True) + EPSILON)
    return (mixed_rows, moved_state * (norm_before / norm_after))


def pass_on(outgoing):
    return passed_along(outgoing, "group", 1)


def body(tokens, learning_rates, channel_gains, fast_init, step_size, update_table):
    start_stream = lax.all_to_all(tokens, "tok", split_axis=1, concat_axis=0, tiled=True)
    group_count = lax.axis_size("group")
    group_index = lax.axis_index("group")
    width_all = start_stream.shape[1] * lax.axis_size("tok")
    layer_count = fast_init.shape[0]
    zero_state = jnp.zeros(fast_init.shape[1:], jnp.float32)

    def tick_work(stream, outgoing, layer_now, active, inverse):
        received = pass_on(outgoing)
        initial = lax.dynamic_index_in_dim(fast_init, layer_now, 0, keepdims=False)
        entering = jnp.where(group_index == 0, initial, received)
        gain_rows = lax.dynamic_index_in_dim(channel_gains, layer_now, 0, keepdims=False)
        rates_row = lax.dynamic_index_in_dim(learning_rates, layer_now, 0, keepdims=False)
        steps_row = lax.dynamic_index_in_dim(step_size, layer_now, 0, keepdims=False)
        table_cell = lax.dynamic_slice(
            update_table, (jnp.asarray(layer_now, jnp.int32), group_index), (1, 1)
        )
        update_flag = table_cell[0, 0].astype(jnp.float32)

        def working(operands):
            return layer_group(
                operands[0], operands[1], gain_rows, rates_row, steps_row, update_flag, inverse
            )

        def resting(operands):
            return (operands[0], operands[2])

        return lax.cond(active, working, resting, (stream, entering, outgoing))

    def one_tick(tick_index, loop_state):
        stream, outgoing = loop_state
        layer_raw = tick_index - group_index
        active = (layer_raw >= 0) & (layer_raw < layer_count)
        layer_now = jnp.clip(layer_raw, 0, layer_count - 1)
        widened = stream.astype(jnp.float32)
        totals = lax.psum(jnp.sum(widened * widened, axis=1), "tok")
        inverse = lax.rsqrt(totals / width_all + EPSILON)
        return tick_work(stream, outgoing, layer_now, active, inverse)

    final_stream, last_state = lax.fori_loop(
        0, layer_count + group_count - 1, one_tick, (start_stream, zero_state)
    )
    return lax.all_to_all(final_stream, "tok", split_axis=0, concat_axis=1, tiled=True)


MESH = pl.DeviceIdType.MESH
F32 = jnp.float32
BF16 = jnp.bfloat16
NN = (((1,), (0,)), ((), ()))
NT = (((1,), (1,)), ((), ()))
TN = (((0,), (0,)), ((), ()))


def dot(a, b, dims=NN):
    return lax.dot_general(a, b, dims, preferred_element_type=F32)


def sigmoid(value):
    return 0.5 * jnp.tanh(0.5 * value) + 0.5


def newton_schulz(values):
    rounded = [v.astype(BF16) for v in values]
    squares = [dot(v, v, NT) for v in rounded]
    narrow = [q.astype(BF16) for q in squares]
    polynoms = [(MUON_B * q + MUON_C * dot(n, n)).astype(BF16) for q, n in zip(squares, narrow)]
    return tuple(MUON_A * v + dot(p, r) for p, v, r in zip(polynoms, values, rounded))


def wave_kernel(
    sizes,
    steps,
    table,
    tokens_in,
    rates_in,
    gains_in,
    initial_in,
    out,
    tokens,
    rates,
    gains,
    initial,
    xin,
    xout,
    weights,
    leaving,
    totals,
    squares,
    partial,
    partials,
    stack,
    grad_gu,
    grad_d,
    t_send,
    t_recv,
    s_send,
    s_recv,
    p_send,
    p_recv,
    w_send,
    w_recv,
    o_send,
    o_recv,
    i_recv,
):
    groups, toks, layers, owned, rows, width, tile = sizes
    group_tok = rows * toks
    g = lax.axis_index("group")
    t = lax.axis_index("tok")
    last = groups - 1

    def remote(source, target, send, recv, to_g, to_t):
        return pltpu.make_async_remote_copy(
            src_ref=source,
            dst_ref=target,
            send_sem=send,
            recv_sem=recv,
            device_id=(to_g, to_t),
            device_id_type=MESH,
        )

    def arrived(target, recv):
        pltpu.make_async_copy(target, target, recv).wait()

    def lane(index, size):
        return pl.ds(pl.multiple_of(index * size, size), size)

    loads = [
        pltpu.make_async_copy(source, target, i_recv.at[i])
        for i, (source, target) in enumerate(
            [(tokens_in, tokens), (rates_in, rates), (gains_in, gains), (initial_in, initial)]
        )
    ]
    for load in loads[:3]:
        load.start()

    @pl.when(g == 0)
    def _():
        loads[3].start()

    barrier = pltpu.get_barrier_semaphore()

    def greet(to_g, to_t):
        pl.semaphore_signal(barrier, inc=1, device_id=(to_g, to_t), device_id_type=MESH)

    chip, core = t // 2, lax.rem(t, 2)
    peers = [
        lax.rem(chip + far, toks // 2) * 2 + side for far in range(1, toks // 2) for side in range(2)
    ] + [t + 1 - 2 * core]
    for to_t in peers:
        greet(g, to_t)

    greet(lax.rem(g + 1, groups), t)
    greet(lax.rem(g + last, groups), t)
    pl.semaphore_wait(barrier, toks + 1)

    def hand_out(j):
        target = xin.at[0, j, lane(t, rows)]
        for i, to_t in enumerate(peers):
            source = tokens.at[:, lane(to_t * owned + j, width)]
            remote(source, target, t_send.at[j, i], t_recv.at[j, t], g, to_t).start()
        source = tokens.at[:, lane(t * owned + j, width)]
        pltpu.make_async_copy(source, target, t_recv.at[j, t]).start()

    loads[0].wait()
    hand_out(0)
    ones_rows = jnp.ones((16, width), BF16)

    def sums_of(values):
        wide = values.astype(F32)
        return dot(ones_rows, (wide * wide).astype(BF16), NT)[0:1]

    totals[...] = jnp.zeros_like(totals)

    @pl.loop(0, owned * toks)
    def _(h):
        totals[...] += sums_of(tokens[:, lane(h, width)])

    squares[t] = totals[...]
    for i, to_t in enumerate(peers):
        remote(totals, squares.at[t], s_send.at[i], s_recv.at[t], g, to_t).start()

    @pl.loop(1, owned)
    def _(j):
        hand_out(j)

    loads[1].wait()
    loads[2].wait()

    @pl.when(g == 0)
    def _():
        loads[3].wait()
        for l in range(layers):
            @pl.loop(0, owned)
            def _(j):
                for which in range(3):
                    weights[l, j, :, which * width : (which + 1) * width] = initial[
                        l, which, j
                    ].astype(BF16)

    pick_row = lax.broadcasted_iota(jnp.int32, (16, 2 * width), 0)
    pick_lane = lax.broadcasted_iota(jnp.int32, (16, 2 * width), 1)
    spread = jnp.where(pick_row // 2 == pick_lane // width, 1.0, 0.0).astype(BF16)

    def scale_rows(l, at, sums):
        size = sums.shape[1]
        inverse = lax.rsqrt(sums / (owned * toks * width) + EPSILON)
        rate = rates[l : l + 1, at]
        inverse_high = inverse.astype(BF16).astype(F32)
        rate_high = rate.astype(BF16).astype(F32)
        at_row = lax.broadcasted_iota(jnp.int32, (16, size), 0)
        fill = jnp.where(at_row == 0, inverse_high, 0.0)
        fill = jnp.where(at_row == 1, inverse - inverse_high, fill)
        fill = jnp.where(at_row == 2, rate_high, fill)
        stack[:, at] = jnp.where(at_row == 3, rate - rate_high, fill).astype(BF16)

    def gains_of(l, j):
        rows_of = gains[l, :, lane(j, width)]
        norm = rows_of[0:1]
        return norm * rows_of[1:2], norm * rows_of[2:3], norm * rows_of[3:4], rows_of[4:5]

    def query(l, j):
        query_gain, _, _, out_gain = gains_of(l, j)
        size = min(tile, group_tok)

        @pl.loop(0, group_tok // size)
        def _(i):
            here = lane(i, size)
            stream = xin[l, j, here, :].astype(F32)
            normed = stream * dot(stack[:, here], spread[:, :width], TN)
            queries = (normed * query_gain).astype(BF16)
            both = dot(queries, weights[l, j, :, : 2 * width])
            gate = both[:, :width]
            hidden = (gate * sigmoid(gate) * both[:, width:]).astype(BF16)
            mixed = (stream + out_gain * dot(hidden, weights[l, j, :, 2 * width :])).astype(BF16)
            if l < layers - 1:
                xin[l + 1, j, here, :] = mixed
                partial[l, :, here] += sums_of(mixed)
            else:
                xout[j, here, :] = mixed

        if l == layers - 1:
            target = out.at[:, lane(t * owned + j, width)]
            for i, to_t in enumerate(peers):
                source = xout.at[j, lane(to_t, rows)]
                remote(source, target, o_send.at[j, i], o_recv, g, to_t).start()
            pltpu.make_async_copy(xout.at[j, lane(t, rows)], target, o_recv).start()

    def learn(l, j):
        _, key_gain, value_gain, _ = gains_of(l, j)
        size = min(tile, group_tok)

        def found(i):
            here = lane(i, size)
            scale = dot(stack[:, here], spread, TN)
            normed = xin[l, j, here, :].astype(F32) * scale[:, :width]
            keys = (normed * key_gain).astype(BF16)
            targets = (normed * value_gain * scale[:, width:]).astype(BF16)
            both = dot(keys, weights[l, j, :, : 2 * width])
            back = dot(targets, weights[l, j, :, 2 * width :], NT)
            gate = both[:, :width]
            up = both[:, width:]
            sig = sigmoid(gate)
            act = gate * sig
            hidden = (act * up).astype(BF16)
            back_up = (back * act).astype(BF16)
            back_gate = (back * up * (sig + act * (1.0 - sig))).astype(BF16)
            backs = jnp.concatenate([back_gate, back_up], axis=1)
            return dot(keys, backs, TN), dot(hidden, targets, TN)

        if size == group_tok:
            return found(0)
        grad_gu[...] = jnp.zeros_like(grad_gu)
        grad_d[...] = jnp.zeros_like(grad_d)

        @pl.loop(0, group_tok // size)
        def _(i):
            more_gu, more_d = found(i)
            grad_gu[...] += more_gu
            grad_d[...] += more_d

        return grad_gu[...], grad_d[...]

    def chain(l, j):
        @pl.when(g > 0)
        def _():
            arrived(weights.at[l, j], w_recv.at[l, j])

        chain_go(l, j)

    def chain_go(l, j):
        @pl.when(g < last)
        def _():
            both, below = learn(l, j)
            grads = (both[:, :width], both[:, width:], below)
            moves = tuple(
                v * lax.rsqrt(jnp.sum(v * v, axis=(0, 1), keepdims=True) + EPSILON) for v in grads
            )
            for _ in range(NS_STEPS):
                moves = newton_schulz(moves)
            step = steps[l, j] * table[l, g].astype(F32)
            for which in range(3):
                at = slice(which * width, (which + 1) * width)
                entering = weights[l, j, :, at].astype(F32)
                moved = entering + step * moves[which]
                before = jnp.sum(entering * entering, axis=0, keepdims=True) + EPSILON
                after = jnp.sum(moved * moved, axis=0, keepdims=True) + EPSILON
                leaving[l, j, :, at] = (moved * (jnp.sqrt(before) * lax.rsqrt(after))).astype(BF16)
            remote(
                leaving.at[l, j], weights.at[l, j], w_send.at[l, j], w_recv.at[l, j], g + 1, t
            ).start()

    def await_tokens(j):
        for k in range(toks):
            arrived(xin.at[0, j, pl.ds(k * rows, rows)], t_recv.at[j, k])

    for to_t in peers:
        arrived(squares.at[to_t], s_recv.at[to_t])
    for k in range(toks):
        scale_rows(0, slice(k * rows, (k + 1) * rows), squares[k])

    for l in range(layers):
        if l > 0:
            arrived_sums = partial[l - 1]
            for to_t in peers:
                arrived(partials.at[l - 1, to_t], p_recv.at[l - 1, to_t])
                arrived_sums += partials[l - 1, to_t]
            scale_rows(l, slice(0, group_tok), arrived_sums)
        if l < layers - 1:
            partial[l] = jnp.zeros((1, group_tok), F32)

            @pl.loop(0, owned - 1)
            def _(j):
                if l == 0:
                    await_tokens(j)
                chain(l, j)
                query(l, j)

            if l == 0:
                await_tokens(owned - 1)

            @pl.when(g > 0)
            def _():
                arrived(weights.at[l, owned - 1], w_recv.at[l, owned - 1])

            query(l, owned - 1)
            for i, to_t in enumerate(peers):
                remote(
                    partial.at[l], partials.at[l, t], p_send.at[l, i], p_recv.at[l, t], g, to_t
                ).start()
            chain_go(l, owned - 1)
        else:
            @pl.loop(0, owned)
            def _(j):
                chain(l, j)

                @pl.when(g == last)
                def _():
                    query(l, j)

            @pl.when(g < last)
            def _():
                @pl.loop(0, owned)
                def _(j):
                    query(l, j)

    arrived(out, o_recv)

    @pl.loop(0, owned)
    def _(j):
        for i, to_t in enumerate(peers):
            arrived(tokens.at[:, lane(to_t * owned + j, width)], t_send.at[j, i])
            arrived(xout.at[j, lane(to_t, rows)], o_send.at[j, i])

        @pl.when(g < last)
        def _():
            for l in range(layers):
                arrived(leaving.at[l, j], w_send.at[l, j])

    for i in range(toks - 1):
        arrived(totals, s_send.at[i])
        for l in range(layers - 1):
            arrived(partial.at[l], p_send.at[l, i])


def wave_body(tokens, learning_rates, channel_gains, fast_init, step_size, update_table):
    groups, toks = lax.axis_size("group"), lax.axis_size("tok")
    layers, _, owned, width, _ = fast_init.shape
    rows, channels = tokens.shape
    group_tok = rows * toks
    sizes = (groups, toks, layers, owned, rows, width, TILE)
    smem = pl.BlockSpec(memory_space=pltpu.SMEM)
    anywhere = pl.BlockSpec(memory_space=pl.ANY)
    dma = pltpu.SemaphoreType.DMA
    return pl.pallas_call(
        functools.partial(wave_kernel, sizes),
        out_shape=jax.ShapeDtypeStruct((rows, channels), BF16),
        in_specs=[smem, smem, anywhere, anywhere, anywhere, anywhere],
        out_specs=anywhere,
        scratch_shapes=[
            pltpu.VMEM(tokens.shape, BF16),
            pltpu.VMEM(learning_rates.shape, F32),
            pltpu.VMEM(channel_gains.shape, F32),
            pltpu.VMEM(fast_init.shape, F32),
            pltpu.VMEM((layers, owned, group_tok, width), BF16),
            pltpu.VMEM((owned, group_tok, width), BF16),
            pltpu.VMEM((layers, owned, width, 3 * width), BF16),
            pltpu.VMEM((layers, owned, width, 3 * width), BF16),
            pltpu.VMEM((1, rows), F32),
            pltpu.VMEM((toks, 1, rows), F32),
            pltpu.VMEM((layers - 1, 1, group_tok), F32),
            pltpu.VMEM((layers - 1, toks, 1, group_tok), F32),
            pltpu.VMEM((16, group_tok), BF16),
            pltpu.VMEM((width, 2 * width), F32),
            pltpu.VMEM((width, width), F32),
            dma((owned, toks)),
            dma((owned, toks)),
            dma((toks,)),
            dma((toks,)),
            dma((layers - 1, toks)),
            dma((layers - 1, toks)),
            dma((layers, owned)),
            dma((layers, owned)),
            dma((owned, toks)),
            dma,
            dma((4,)),
        ],
        compiler_params=pltpu.CompilerParams(
            collective_id=0, has_side_effects=True, vmem_limit_bytes=48 * 1024 * 1024
        ),
    )(step_size, update_table, tokens, learning_rates, channel_gains, fast_init)


TILE = 2048


def plan(mesh, tokens, fast_init):
    groups, toks = mesh.shape["group"], mesh.shape["tok"]
    layers, _, heads, width, _ = fast_init.shape
    rows = tokens.shape[0] // (groups * toks)
    fits = groups > 1 and toks > 2 and toks % 2 == 0 and layers > 1 and heads % toks == 0
    fits = fits and rows * toks % TILE == 0 and rows % 128 == 0 and width % 128 == 0
    return wave_body if fits and tokens.shape[0] * tokens.shape[1] <= 64 * 1024 * 1024 else body


def solution(mesh):
    in_specs = (
        P(("group", "tok"), None),
        P(None, "group"),
        P(None, None, "tok"),
        P(None, None, "tok", None, None),
        P(None, "tok"),
        P(),
    )
    out_specs = P(("group", "tok"), None)
    def run(*args):
        chosen = plan(mesh, args[0], args[3])
        return jax.shard_map(
            chosen, mesh=mesh, in_specs=in_specs, out_specs=out_specs, check_vma=False
        )(*args)

    return run
```

```python
import functools

import jax
import jax.numpy as jnp
from jax import lax
from jax.experimental import pallas as pl
from jax.experimental.pallas import tpu as pltpu
from jax.sharding import PartitionSpec as P

NS_STEPS = 5


MUON_A = 3.4445
MUON_B = -4.775
MUON_C = 2.0315
EPSILON = 1e-06


def passed_along(value, axis, by):
    size = lax.axis_size(axis)
    pairs = [(i, i + by) for i in range(size) if 0 <= i + by < size]
    return lax.ppermute(value, axis, pairs)


def orthogonalize(gradient):
    scaling = lax.rsqrt(jnp.sum(gradient * gradient, axis=(-2, -1), keepdims=True) + EPSILON)
    current = gradient * scaling
    for repeat in range(NS_STEPS):
        square = jnp.einsum("...ij,...kj->...ik", current, current, precision=lax.Precision.HIGHEST)
        polynom = MUON_B * square + MUON_C * jnp.einsum(
            "...ij,...jk->...ik", square, square, precision=lax.Precision.HIGHEST
        )
        current = MUON_A * current + jnp.einsum(
            "...ij,...jk->...ik", polynom, current, precision=lax.Precision.HIGHEST
        )
    return current


def layer_group(stream, entering, gain_rows, rates_row, steps_row, update_flag, inverse):
    row_count, channel_count = stream.shape
    heads_n = entering.shape[1]
    head_dim = entering.shape[2]
    normed = stream.astype(jnp.float32) * inverse[:, None] * gain_rows[0]
    queries = (normed * gain_rows[1]).astype(jnp.bfloat16).reshape(row_count, heads_n, head_dim)
    keys_in = (normed * gain_rows[2]).astype(jnp.bfloat16).reshape(row_count, heads_n, head_dim)
    values_in = (normed * gain_rows[3]).astype(jnp.bfloat16).reshape(row_count, heads_n, head_dim)
    rounded = entering.astype(jnp.bfloat16)
    gate_q = jnp.einsum("thi,hij->thj", queries, rounded[0], preferred_element_type=jnp.float32)
    up_q = jnp.einsum("thi,hij->thj", queries, rounded[1], preferred_element_type=jnp.float32)
    hidden_q = (jax.nn.silu(gate_q) * up_q).astype(jnp.bfloat16)
    output = jnp.einsum(
        "thj,hjk->thk", hidden_q, rounded[2], preferred_element_type=jnp.float32
    ).reshape(row_count, channel_count)
    mixed_rows = (stream.astype(jnp.float32) + gain_rows[4] * output).astype(jnp.bfloat16)
    gate_k = jnp.einsum("thi,hij->thj", keys_in, rounded[0], preferred_element_type=jnp.float32)
    up_k = jnp.einsum("thi,hij->thj", keys_in, rounded[1], preferred_element_type=jnp.float32)
    sigmoid_k = jax.nn.sigmoid(gate_k)
    active_k = gate_k * sigmoid_k
    hidden_k = (active_k * up_k).astype(jnp.bfloat16)
    targets = (rates_row[:, None, None] * values_in.astype(jnp.float32)).astype(jnp.bfloat16)
    back_hidden = jnp.einsum(
        "thk,hjk->thj", targets, rounded[2], preferred_element_type=jnp.float32
    )
    back_up = (back_hidden * active_k).astype(jnp.bfloat16)
    back_gate = (back_hidden * up_k * sigmoid_k * (1.0 + gate_k * (1.0 - sigmoid_k))).astype(
        jnp.bfloat16
    )
    grad_gate = jnp.einsum("thi,thj->hij", keys_in, back_gate, preferred_element_type=jnp.float32)
    grad_up = jnp.einsum("thi,thj->hij", keys_in, back_up, preferred_element_type=jnp.float32)
    grad_down = jnp.einsum("thj,thk->hjk", hidden_k, targets, preferred_element_type=jnp.float32)
    direction = orthogonalize(jnp.stack([grad_gate, grad_up, grad_down]))
    moved_state = entering + (update_flag * steps_row)[None, :, None, None] * direction
    norm_before = jnp.sqrt(jnp.sum(entering * entering, axis=2, keepdims=True) + EPSILON)
    norm_after = jnp.sqrt(jnp.sum(moved_state * moved_state, axis=2, keepdims=True) + EPSILON)
    return (mixed_rows, moved_state * (norm_before / norm_after))


def pass_on(outgoing):
    return passed_along(outgoing, "group", 1)


def body(tokens, learning_rates, channel_gains, fast_init, step_size, update_table):
    start_stream = lax.all_to_all(tokens, "tok", split_axis=1, concat_axis=0, tiled=True)
    group_count = lax.axis_size("group")
    group_index = lax.axis_index("group")
    width_all = start_stream.shape[1] * lax.axis_size("tok")
    layer_count = fast_init.shape[0]
    zero_state = jnp.zeros(fast_init.shape[1:], jnp.float32)

    def tick_work(stream, outgoing, layer_now, active, inverse):
        received = pass_on(outgoing)
        initial = lax.dynamic_index_in_dim(fast_init, layer_now, 0, keepdims=False)
        entering = jnp.where(group_index == 0, initial, received)
        gain_rows = lax.dynamic_index_in_dim(channel_gains, layer_now, 0, keepdims=False)
        rates_row = lax.dynamic_index_in_dim(learning_rates, layer_now, 0, keepdims=False)
        steps_row = lax.dynamic_index_in_dim(step_size, layer_now, 0, keepdims=False)
        table_cell = lax.dynamic_slice(
            update_table, (jnp.asarray(layer_now, jnp.int32), group_index), (1, 1)
        )
        update_flag = table_cell[0, 0].astype(jnp.float32)

        def working(operands):
            return layer_group(
                operands[0], operands[1], gain_rows, rates_row, steps_row, update_flag, inverse
            )

        def resting(operands):
            return (operands[0], operands[2])

        return lax.cond(active, working, resting, (stream, entering, outgoing))

    def one_tick(tick_index, loop_state):
        stream, outgoing = loop_state
        layer_raw = tick_index - group_index
        active = (layer_raw >= 0) & (layer_raw < layer_count)
        layer_now = jnp.clip(layer_raw, 0, layer_count - 1)
        widened = stream.astype(jnp.float32)
        totals = lax.psum(jnp.sum(widened * widened, axis=1), "tok")
        inverse = lax.rsqrt(totals / width_all + EPSILON)
        return tick_work(stream, outgoing, layer_now, active, inverse)

    final_stream, last_state = lax.fori_loop(
        0, layer_count + group_count - 1, one_tick, (start_stream, zero_state)
    )
    return lax.all_to_all(final_stream, "tok", split_axis=0, concat_axis=1, tiled=True)


MESH = pl.DeviceIdType.MESH
F32 = jnp.float32
BF16 = jnp.bfloat16
NN = (((1,), (0,)), ((), ()))
NT = (((1,), (1,)), ((), ()))
TN = (((0,), (0,)), ((), ()))


def dot(a, b, dims=NN):
    return lax.dot_general(a, b, dims, preferred_element_type=F32)


def halves(value):
    high = value.astype(BF16)
    return high, (value - high.astype(F32)).astype(BF16)


def product(a, b):
    a_high, a_low = halves(a)
    b_high, b_low = halves(b)
    left = jnp.concatenate([a_high, a_low], axis=1)
    above = jnp.concatenate([b_high, b_low], axis=1)
    below = jnp.concatenate([b_high, jnp.zeros_like(b_low)], axis=1)
    both = dot(left, jnp.concatenate([above, below], axis=0))
    return both[:, : b.shape[1]] + both[:, b.shape[1] :]


def sigmoid(value):
    return 0.5 * jnp.tanh(0.5 * value) + 0.5


def coarse(a, b):
    return dot(a.astype(BF16), b.astype(BF16))


def newton_schulz(values, times):
    rounded = [v.astype(BF16) for v in values]
    squares = [dot(v, v, NT) for v in rounded]
    polynoms = [MUON_B * q + MUON_C * times(q, q) for q in squares]
    return tuple(MUON_A * v + times(p, v) for p, v in zip(polynoms, values))


def wave_kernel(
    sizes,
    steps_in,
    table_in,
    tokens_in,
    rates_in,
    gains_in,
    initial_in,
    out,
    steps,
    table,
    tokens,
    rates,
    gains,
    initial,
    xin,
    xout,
    weights,
    leaving,
    totals,
    squares,
    partial,
    partials,
    stack,
    grad_gu,
    grad_d,
    t_send,
    t_recv,
    s_send,
    s_recv,
    p_send,
    p_recv,
    w_send,
    w_recv,
    o_send,
    o_recv,
    i_recv,
    passing,
    q_send,
    q_recv,
):
    groups, toks, layers, owned, rows, width, tile = sizes
    group_tok = rows * toks
    g = lax.axis_index("group")
    t = lax.axis_index("tok")
    last = groups - 1

    def remote(source, target, send, recv, to_g, to_t):
        return pltpu.make_async_remote_copy(
            src_ref=source,
            dst_ref=target,
            send_sem=send,
            recv_sem=recv,
            device_id=(to_g, to_t),
            device_id_type=MESH,
        )

    def arrived(target, recv):
        pltpu.make_async_copy(target, target, recv).wait()

    def lane(index, size):
        return pl.ds(pl.multiple_of(index * size, size), size)

    loads = [
        pltpu.make_async_copy(source, target, i_recv.at[i])
        for i, (source, target) in enumerate(
            [
                (tokens_in, tokens),
                (rates_in, rates),
                (gains_in, gains),
                (steps_in, steps),
                (table_in, table),
                (initial_in, initial),
            ]
        )
    ]
    for load in loads[:5]:
        load.start()

    @pl.when(g == 0)
    def _():
        loads[5].start()

    barrier = pltpu.get_barrier_semaphore()

    def greet(to_g, to_t):
        pl.semaphore_signal(barrier, inc=1, device_id=(to_g, to_t), device_id_type=MESH)

    chip, core = t // 2, lax.rem(t, 2)
    peers = [
        lax.rem(chip + far, toks // 2) * 2 + side for far in range(1, toks // 2) for side in range(2)
    ] + [t + 1 - 2 * core]
    for to_t in peers:
        greet(g, to_t)

    greet(lax.rem(g + 1, groups), t)
    greet(lax.rem(g + last, groups), t)
    far = toks - 2
    for away in (2, groups - 2):
        near_g = lax.rem(g + away, groups)
        greet(near_g, t)
        for to_t in peers[:far]:
            greet(near_g, to_t)
    pl.semaphore_wait(barrier, toks + 3 + 2 * far)
    relays = (groups - 3, 1)
    share = rows // 64 * 16
    kept = rows - 2 * share

    def hand_out(j):
        target = xin.at[0, j, lane(t, rows)]
        for i, to_t in enumerate(peers):
            source = tokens.at[:, lane(to_t * owned + j, width)]
            remote(source, target, t_send.at[j, i], t_recv.at[j, t], g, to_t).start()
        source = tokens.at[:, lane(t * owned + j, width)]
        pltpu.make_async_copy(source, target, t_recv.at[j, t]).start()

    loads[0].wait()
    hand_out(0)
    ones_rows = jnp.ones((16, width), BF16)

    def sums_of(values):
        wide = values.astype(F32)
        return dot(ones_rows, (wide * wide).astype(BF16), NT)[0:1]

    totals[...] = jnp.zeros_like(totals)

    @pl.loop(0, owned * toks)
    def _(h):
        totals[...] += sums_of(tokens[:, lane(h, width)])

    squares[t] = totals[...]
    for i, to_t in enumerate(peers):
        remote(totals, squares.at[t], s_send.at[i], s_recv.at[t], g, to_t).start()

    @pl.loop(1, owned)
    def _(j):
        hand_out(j)

    for load in loads[1:5]:
        load.wait()

    @pl.when(g == 0)
    def _():
        loads[5].wait()
        for l in range(layers):
            @pl.loop(0, owned)
            def _(j):
                for which in range(3):
                    weights[l, j, :, which * width : (which + 1) * width] = initial[
                        l, which, j
                    ].astype(BF16)

    pick_row = lax.broadcasted_iota(jnp.int32, (16, 2 * width), 0)
    pick_lane = lax.broadcasted_iota(jnp.int32, (16, 2 * width), 1)
    spread = jnp.where(pick_row // 2 == pick_lane // width, 1.0, 0.0).astype(BF16)

    def scale_rows(l, at, sums):
        size = sums.shape[1]
        inverse = lax.rsqrt(sums / (owned * toks * width) + EPSILON)
        rate = rates[l : l + 1, at]
        inverse_high = inverse.astype(BF16).astype(F32)
        rate_high = rate.astype(BF16).astype(F32)
        at_row = lax.broadcasted_iota(jnp.int32, (16, size), 0)
        fill = jnp.where(at_row == 0, inverse_high, 0.0)
        fill = jnp.where(at_row == 1, inverse - inverse_high, fill)
        fill = jnp.where(at_row == 2, rate_high, fill)
        stack[:, at] = jnp.where(at_row == 3, rate - rate_high, fill).astype(BF16)

    def gains_of(l, j):
        rows_of = gains[:, l, lane(j, width)]
        norm = rows_of[0:1]
        return norm * rows_of[1:2], norm * rows_of[2:3], norm * rows_of[3:4], rows_of[4:5]

    def query(l, j):
        query_gain, _, _, out_gain = gains_of(l, j)
        size = min(tile, group_tok)

        @pl.loop(0, group_tok // size)
        def _(i):
            here = lane(i, size)
            stream = xin[l, j, here, :].astype(F32)
            normed = stream * dot(stack[:, here], spread[:, :width], TN)
            queries = (normed * query_gain).astype(BF16)
            both = dot(queries, weights[l, j, :, : 2 * width])
            gate = both[:, :width]
            hidden = (gate * sigmoid(gate) * both[:, width:]).astype(BF16)
            mixed = (stream + out_gain * dot(hidden, weights[l, j, :, 2 * width :])).astype(BF16)
            if l < layers - 1:
                xin[l + 1, j, here, :] = mixed
                partial[l, :, here] += sums_of(mixed)
            else:
                xout[j, here, :] = mixed

        if l == layers - 1:
            target = out.at[:, lane(t * owned + j, width)]

            @pl.when(g < last)
            def _():
                for i, to_t in enumerate(peers):
                    source = xout.at[j, lane(to_t, rows)]
                    remote(source, target, o_send.at[j, i], o_recv, g, to_t).start()

            @pl.when(g == last)
            def _():
                for i, to_t in enumerate(peers[:far]):
                    for r, relay in enumerate(relays):
                        source = xout.at[j, pl.ds(to_t * rows + kept + r * share, share)]
                        remote(
                            source, passing.at[j, i], q_send.at[r, j, i], q_recv.at[j, i], relay, t
                        ).start()
                for i, to_t in enumerate(peers[:far]):
                    source = xout.at[j, pl.ds(to_t * rows, kept)]
                    remote(source, target.at[:kept], o_send.at[j, i], o_recv, g, to_t).start()
                source = xout.at[j, lane(peers[far], rows)]
                remote(source, target, o_send.at[j, far], o_recv, g, peers[far]).start()

            pltpu.make_async_copy(xout.at[j, lane(t, rows)], target, o_recv).start()

    def learn(l, j):
        _, key_gain, value_gain, _ = gains_of(l, j)
        size = min(tile, group_tok)

        def found(i):
            here = lane(i, size)
            scale = dot(stack[:, here], spread, TN)
            normed = xin[l, j, here, :].astype(F32) * scale[:, :width]
            keys = (normed * key_gain).astype(BF16)
            targets = (normed * value_gain * scale[:, width:]).astype(BF16)
            both = dot(keys, weights[l, j, :, : 2 * width])
            back = dot(targets, weights[l, j, :, 2 * width :], NT)
            gate = both[:, :width]
            up = both[:, width:]
            sig = sigmoid(gate)
            act = gate * sig
            hidden = (act * up).astype(BF16)
            back_up = (back * act).astype(BF16)
            back_gate = (back * up * (sig + act * (1.0 - sig))).astype(BF16)
            backs = jnp.concatenate([back_gate, back_up], axis=1)
            return dot(keys, backs, TN), dot(hidden, targets, TN)

        if size == group_tok:
            return found(0)
        grad_gu[...] = jnp.zeros_like(grad_gu)
        grad_d[...] = jnp.zeros_like(grad_d)

        @pl.loop(0, group_tok // size)
        def _(i):
            more_gu, more_d = found(i)
            grad_gu[...] += more_gu
            grad_d[...] += more_d

        return grad_gu[...], grad_d[...]

    def chain(l, j):
        @pl.when(g > 0)
        def _():
            arrived(weights.at[l, j], w_recv.at[l, j])

        chain_go(l, j)

    def chain_go(l, j):
        @pl.when(g < last)
        def _():
            both, below = learn(l, j)
            grads = (both[:, :width], both[:, width:], below)
            moves = tuple(
                v * lax.rsqrt(jnp.sum(v * v, axis=(0, 1), keepdims=True) + EPSILON) for v in grads
            )
            for repeat in range(NS_STEPS):
                moves = newton_schulz(moves, coarse if repeat < 2 else product)
            step = steps[l, j] * table[l, g].astype(F32)
            for which in range(3):
                at = slice(which * width, (which + 1) * width)
                entering = weights[l, j, :, at].astype(F32)
                moved = entering + step * moves[which]
                before = jnp.sum(entering * entering, axis=0, keepdims=True) + EPSILON
                after = jnp.sum(moved * moved, axis=0, keepdims=True) + EPSILON
                leaving[l, j, :, at] = (moved * (jnp.sqrt(before) * lax.rsqrt(after))).astype(BF16)
            remote(
                leaving.at[l, j], weights.at[l, j], w_send.at[l, j], w_recv.at[l, j], g + 1, t
            ).start()

    def await_tokens(j):
        for k in range(toks):
            arrived(xin.at[0, j, pl.ds(k * rows, rows)], t_recv.at[j, k])

    for to_t in peers:
        arrived(squares.at[to_t], s_recv.at[to_t])
    for k in range(toks):
        scale_rows(0, slice(k * rows, (k + 1) * rows), squares[k])

    for l in range(layers):
        if l > 0:
            arrived_sums = partial[l - 1]
            for to_t in peers:
                arrived(partials.at[l - 1, to_t], p_recv.at[l - 1, to_t])
                arrived_sums += partials[l - 1, to_t]
            scale_rows(l, slice(0, group_tok), arrived_sums)
        if l < layers - 1:
            partial[l] = jnp.zeros((1, group_tok), F32)

            @pl.loop(0, owned - 1)
            def _(j):
                if l == 0:
                    await_tokens(j)
                chain(l, j)
                query(l, j)

            if l == 0:
                await_tokens(owned - 1)

            @pl.when(g > 0)
            def _():
                arrived(weights.at[l, owned - 1], w_recv.at[l, owned - 1])

            query(l, owned - 1)
            for i, to_t in enumerate(peers):
                remote(
                    partial.at[l], partials.at[l, t], p_send.at[l, i], p_recv.at[l, t], g, to_t
                ).start()
            chain_go(l, owned - 1)
        else:
            @pl.loop(0, owned)
            def _(j):
                chain(l, j)

                @pl.when(g == last)
                def _():
                    query(l, j)

            @pl.when(g < last)
            def _():
                @pl.loop(0, owned)
                def _(j):
                    query(l, j)

    for r, relay in enumerate(relays):

        @pl.when(g == relay)
        def _():
            @pl.loop(0, owned)
            def _(j):
                for i, to_t in enumerate(peers[:far]):
                    arrived(passing.at[j, i], q_recv.at[j, i])
                    target = out.at[pl.ds(kept + r * share, share), lane(t * owned + j, width)]
                    remote(
                        passing.at[j, i], target, q_send.at[r, j, i], o_recv, last, to_t
                    ).start()

            @pl.loop(0, owned)
            def _(j):
                for i in range(far):
                    arrived(passing.at[j, i], q_send.at[r, j, i])

    arrived(out, o_recv)

    @pl.loop(0, owned)
    def _(j):
        for i, to_t in enumerate(peers):
            arrived(tokens.at[:, lane(to_t * owned + j, width)], t_send.at[j, i])

            @pl.when(g < last)
            def _():
                arrived(xout.at[j, lane(to_t, rows)], o_send.at[j, i])

        @pl.when(g == last)
        def _():
            for i in range(far):
                arrived(xout.at[j, :kept], o_send.at[j, i])
                for r in range(2):
                    arrived(passing.at[j, i], q_send.at[r, j, i])
            arrived(xout.at[j, :rows], o_send.at[j, far])

        @pl.when(g < last)
        def _():
            for l in range(layers):
                arrived(leaving.at[l, j], w_send.at[l, j])

    for i in range(toks - 1):
        arrived(totals, s_send.at[i])
        for l in range(layers - 1):
            arrived(partial.at[l], p_send.at[l, i])


def wave_body(tokens, learning_rates, channel_gains, fast_init, step_size, update_table):
    groups, toks = lax.axis_size("group"), lax.axis_size("tok")
    layers, _, owned, width, _ = fast_init.shape
    rows, channels = tokens.shape
    group_tok = rows * toks
    gains = channel_gains.transpose(1, 0, 2)
    sizes = (groups, toks, layers, owned, rows, width, TILE)
    anywhere = pl.BlockSpec(memory_space=pl.ANY)
    dma = pltpu.SemaphoreType.DMA
    return pl.pallas_call(
        functools.partial(wave_kernel, sizes),
        out_shape=jax.ShapeDtypeStruct((rows, channels), BF16),
        in_specs=[anywhere] * 6,
        out_specs=anywhere,
        scratch_shapes=[
            pltpu.SMEM(step_size.shape, F32),
            pltpu.SMEM(update_table.shape, jnp.int32),
            pltpu.VMEM(tokens.shape, BF16),
            pltpu.VMEM(learning_rates.shape, F32),
            pltpu.VMEM(gains.shape, F32),
            pltpu.VMEM(fast_init.shape, F32),
            pltpu.VMEM((layers, owned, group_tok, width), BF16),
            pltpu.VMEM((owned, group_tok, width), BF16),
            pltpu.VMEM((layers, owned, width, 3 * width), BF16),
            pltpu.VMEM((layers, owned, width, 3 * width), BF16),
            pltpu.VMEM((1, rows), F32),
            pltpu.VMEM((toks, 1, rows), F32),
            pltpu.VMEM((layers - 1, 1, group_tok), F32),
            pltpu.VMEM((layers - 1, toks, 1, group_tok), F32),
            pltpu.VMEM((16, group_tok), BF16),
            pltpu.VMEM((width, 2 * width), F32),
            pltpu.VMEM((width, width), F32),
            dma((owned, toks)),
            dma((owned, toks)),
            dma((toks,)),
            dma((toks,)),
            dma((layers - 1, toks)),
            dma((layers - 1, toks)),
            dma((layers, owned)),
            dma((layers, owned)),
            dma((owned, toks)),
            dma,
            dma((6,)),
            pltpu.VMEM((owned, toks - 2, rows // 64 * 16, width), BF16),
            dma((2, owned, toks - 2)),
            dma((owned, toks - 2)),
        ],
        compiler_params=pltpu.CompilerParams(
            collective_id=0, has_side_effects=True, vmem_limit_bytes=VMEM_LIMIT
        ),
    )(step_size, update_table, tokens, learning_rates, gains, fast_init)


TILE = 2048
VMEM_LIMIT = 67_043_328


def plan(mesh, tokens, fast_init):
    groups, toks = mesh.shape["group"], mesh.shape["tok"]
    layers, _, heads, width, _ = fast_init.shape
    rows = tokens.shape[0] // (groups * toks)
    fits = groups > 4 and toks > 2 and toks % 2 == 0 and layers > 1 and heads % toks == 0
    fits = fits and rows * toks % TILE == 0 and rows % 128 == 0 and width % 128 == 0
    return wave_body if fits and tokens.shape[0] * tokens.shape[1] <= 64 * 1024 * 1024 else body


def solution(mesh):
    in_specs = (
        P(("group", "tok"), None),
        P(None, "group"),
        P(None, None, "tok"),
        P(None, None, "tok", None, None),
        P(None, "tok"),
        P(),
    )
    out_specs = P(("group", "tok"), None)
    def run(*args):
        chosen = plan(mesh, args[0], args[3])
        return jax.shard_map(
            chosen, mesh=mesh, in_specs=in_specs, out_specs=out_specs, check_vma=False
        )(*args)

    return run
```

```python
import functools

import jax
import jax.numpy as jnp
from jax import lax
from jax.experimental import pallas as pl
from jax.experimental.pallas import tpu as pltpu
from jax.sharding import PartitionSpec as P

NS_STEPS = 5


MUON_A = 3.4445
MUON_B = -4.775
MUON_C = 2.0315
EPSILON = 1e-06


def passed_along(value, axis, by):
    size = lax.axis_size(axis)
    pairs = [(i, i + by) for i in range(size) if 0 <= i + by < size]
    return lax.ppermute(value, axis, pairs)


def orthogonalize(gradient):
    scaling = lax.rsqrt(jnp.sum(gradient * gradient, axis=(-2, -1), keepdims=True) + EPSILON)
    current = gradient * scaling
    for repeat in range(NS_STEPS):
        square = jnp.einsum("...ij,...kj->...ik", current, current, precision=lax.Precision.HIGHEST)
        polynom = MUON_B * square + MUON_C * jnp.einsum(
            "...ij,...jk->...ik", square, square, precision=lax.Precision.HIGHEST
        )
        current = MUON_A * current + jnp.einsum(
            "...ij,...jk->...ik", polynom, current, precision=lax.Precision.HIGHEST
        )
    return current


def layer_group(stream, entering, gain_rows, rates_row, steps_row, update_flag, inverse):
    row_count, channel_count = stream.shape
    heads_n = entering.shape[1]
    head_dim = entering.shape[2]
    normed = stream.astype(jnp.float32) * inverse[:, None] * gain_rows[0]
    queries = (normed * gain_rows[1]).astype(jnp.bfloat16).reshape(row_count, heads_n, head_dim)
    keys_in = (normed * gain_rows[2]).astype(jnp.bfloat16).reshape(row_count, heads_n, head_dim)
    values_in = (normed * gain_rows[3]).astype(jnp.bfloat16).reshape(row_count, heads_n, head_dim)
    rounded = entering.astype(jnp.bfloat16)
    gate_q = jnp.einsum("thi,hij->thj", queries, rounded[0], preferred_element_type=jnp.float32)
    up_q = jnp.einsum("thi,hij->thj", queries, rounded[1], preferred_element_type=jnp.float32)
    hidden_q = (jax.nn.silu(gate_q) * up_q).astype(jnp.bfloat16)
    output = jnp.einsum(
        "thj,hjk->thk", hidden_q, rounded[2], preferred_element_type=jnp.float32
    ).reshape(row_count, channel_count)
    mixed_rows = (stream.astype(jnp.float32) + gain_rows[4] * output).astype(jnp.bfloat16)
    gate_k = jnp.einsum("thi,hij->thj", keys_in, rounded[0], preferred_element_type=jnp.float32)
    up_k = jnp.einsum("thi,hij->thj", keys_in, rounded[1], preferred_element_type=jnp.float32)
    sigmoid_k = jax.nn.sigmoid(gate_k)
    active_k = gate_k * sigmoid_k
    hidden_k = (active_k * up_k).astype(jnp.bfloat16)
    targets = (rates_row[:, None, None] * values_in.astype(jnp.float32)).astype(jnp.bfloat16)
    back_hidden = jnp.einsum(
        "thk,hjk->thj", targets, rounded[2], preferred_element_type=jnp.float32
    )
    back_up = (back_hidden * active_k).astype(jnp.bfloat16)
    back_gate = (back_hidden * up_k * sigmoid_k * (1.0 + gate_k * (1.0 - sigmoid_k))).astype(
        jnp.bfloat16
    )
    grad_gate = jnp.einsum("thi,thj->hij", keys_in, back_gate, preferred_element_type=jnp.float32)
    grad_up = jnp.einsum("thi,thj->hij", keys_in, back_up, preferred_element_type=jnp.float32)
    grad_down = jnp.einsum("thj,thk->hjk", hidden_k, targets, preferred_element_type=jnp.float32)
    direction = orthogonalize(jnp.stack([grad_gate, grad_up, grad_down]))
    moved_state = entering + (update_flag * steps_row)[None, :, None, None] * direction
    norm_before = jnp.sqrt(jnp.sum(entering * entering, axis=2, keepdims=True) + EPSILON)
    norm_after = jnp.sqrt(jnp.sum(moved_state * moved_state, axis=2, keepdims=True) + EPSILON)
    return (mixed_rows, moved_state * (norm_before / norm_after))


def pass_on(outgoing):
    return passed_along(outgoing, "group", 1)


def body(tokens, learning_rates, channel_gains, fast_init, step_size, update_table):
    start_stream = lax.all_to_all(tokens, "tok", split_axis=1, concat_axis=0, tiled=True)
    group_count = lax.axis_size("group")
    group_index = lax.axis_index("group")
    width_all = start_stream.shape[1] * lax.axis_size("tok")
    layer_count = fast_init.shape[0]
    zero_state = jnp.zeros(fast_init.shape[1:], jnp.float32)

    def tick_work(stream, outgoing, layer_now, active, inverse):
        received = pass_on(outgoing)
        initial = lax.dynamic_index_in_dim(fast_init, layer_now, 0, keepdims=False)
        entering = jnp.where(group_index == 0, initial, received)
        gain_rows = lax.dynamic_index_in_dim(channel_gains, layer_now, 0, keepdims=False)
        rates_row = lax.dynamic_index_in_dim(learning_rates, layer_now, 0, keepdims=False)
        steps_row = lax.dynamic_index_in_dim(step_size, layer_now, 0, keepdims=False)
        table_cell = lax.dynamic_slice(
            update_table, (jnp.asarray(layer_now, jnp.int32), group_index), (1, 1)
        )
        update_flag = table_cell[0, 0].astype(jnp.float32)

        def working(operands):
            return layer_group(
                operands[0], operands[1], gain_rows, rates_row, steps_row, update_flag, inverse
            )

        def resting(operands):
            return (operands[0], operands[2])

        return lax.cond(active, working, resting, (stream, entering, outgoing))

    def one_tick(tick_index, loop_state):
        stream, outgoing = loop_state
        layer_raw = tick_index - group_index
        active = (layer_raw >= 0) & (layer_raw < layer_count)
        layer_now = jnp.clip(layer_raw, 0, layer_count - 1)
        widened = stream.astype(jnp.float32)
        totals = lax.psum(jnp.sum(widened * widened, axis=1), "tok")
        inverse = lax.rsqrt(totals / width_all + EPSILON)
        return tick_work(stream, outgoing, layer_now, active, inverse)

    final_stream, last_state = lax.fori_loop(
        0, layer_count + group_count - 1, one_tick, (start_stream, zero_state)
    )
    return lax.all_to_all(final_stream, "tok", split_axis=0, concat_axis=1, tiled=True)


MESH = pl.DeviceIdType.MESH
F32 = jnp.float32
BF16 = jnp.bfloat16
NN = (((1,), (0,)), ((), ()))
NT = (((1,), (1,)), ((), ()))
TN = (((0,), (0,)), ((), ()))


def dot(a, b, dims=NN):
    return lax.dot_general(a, b, dims, preferred_element_type=F32)


def halves(value):
    high = value.astype(BF16)
    return high, (value - high.astype(F32)).astype(BF16)


def product(a, b):
    a_high, a_low = halves(a)
    b_high, b_low = halves(b)
    left = jnp.concatenate([a_high, a_low], axis=1)
    above = jnp.concatenate([b_high, b_low], axis=1)
    below = jnp.concatenate([b_high, jnp.zeros_like(b_low)], axis=1)
    both = dot(left, jnp.concatenate([above, below], axis=0))
    return both[:, : b.shape[1]] + both[:, b.shape[1] :]


def sigmoid(value):
    return 0.5 * jnp.tanh(0.5 * value) + 0.5


def coarse(a, b):
    return dot(a.astype(BF16), b.astype(BF16))


def newton_schulz(values, times):
    rounded = [v.astype(BF16) for v in values]
    squares = [dot(v, v, NT) for v in rounded]
    polynoms = [MUON_B * q + MUON_C * times(q, q) for q in squares]
    return tuple(MUON_A * v + times(p, v) for p, v in zip(polynoms, values))


def wave_kernel(
    sizes,
    steps_in,
    table_in,
    tokens_in,
    rates_in,
    gains_in,
    initial_in,
    out,
    steps,
    table,
    tokens,
    rates,
    gains,
    initial,
    xin,
    xout,
    weights,
    leaving,
    totals,
    squares,
    partial,
    partials,
    stack,
    grad_gu,
    grad_d,
    t_send,
    t_recv,
    s_send,
    s_recv,
    p_send,
    p_recv,
    w_send,
    w_recv,
    o_send,
    o_recv,
    i_recv,
    passing,
    q_send,
    q_recv,
):
    groups, toks, layers, owned, rows, width, tile = sizes
    group_tok = rows * toks
    g = lax.axis_index("group")
    t = lax.axis_index("tok")
    last = groups - 1

    def remote(source, target, send, recv, to_g, to_t):
        return pltpu.make_async_remote_copy(
            src_ref=source,
            dst_ref=target,
            send_sem=send,
            recv_sem=recv,
            device_id=(to_g, to_t),
            device_id_type=MESH,
        )

    def arrived(target, recv):
        pltpu.make_async_copy(target, target, recv).wait()

    def lane(index, size):
        return pl.ds(pl.multiple_of(index * size, size), size)

    loads = [
        pltpu.make_async_copy(source, target, i_recv.at[i])
        for i, (source, target) in enumerate(
            [
                (tokens_in, tokens),
                (rates_in, rates),
                (gains_in, gains),
                (steps_in, steps),
                (table_in, table),
                (initial_in, initial),
            ]
        )
    ]
    for load in loads[:5]:
        load.start()

    @pl.when(g == 0)
    def _():
        loads[5].start()

    barrier = pltpu.get_barrier_semaphore()

    def greet(to_g, to_t):
        pl.semaphore_signal(barrier, inc=1, device_id=(to_g, to_t), device_id_type=MESH)

    chip, core = t // 2, lax.rem(t, 2)
    peers = [
        lax.rem(chip + far, toks // 2) * 2 + side for far in range(1, toks // 2) for side in range(2)
    ] + [t + 1 - 2 * core]
    for to_t in peers:
        greet(g, to_t)

    greet(lax.rem(g + 1, groups), t)
    greet(lax.rem(g + last, groups), t)
    far = toks - 2
    for away in (2, groups - 2):
        near_g = lax.rem(g + away, groups)
        greet(near_g, t)
        for to_t in peers[:far]:
            greet(near_g, to_t)
    pl.semaphore_wait(barrier, toks + 3 + 2 * far)
    share = passing.shape[2]
    kept = rows - share
    late = g >= groups - 2
    at_once = owned // 2

    def hand_out(j):
        target = xin.at[0, j, lane(t, rows)]
        for i, to_t in enumerate(peers):
            source = tokens.at[:, lane(to_t * owned + j, width)]
            remote(source, target, t_send.at[j, i], t_recv.at[j, t], g, to_t).start()
        source = tokens.at[:, lane(t * owned + j, width)]
        pltpu.make_async_copy(source, target, t_recv.at[j, t]).start()

    loads[0].wait()
    hand_out(0)
    ones_rows = jnp.ones((16, width), BF16)

    def sums_of(values):
        wide = values.astype(F32)
        return dot(ones_rows, (wide * wide).astype(BF16), NT)[0:1]

    totals[...] = jnp.zeros_like(totals)

    @pl.loop(0, owned * toks)
    def _(h):
        totals[...] += sums_of(tokens[:, lane(h, width)])

    squares[t] = totals[...]
    for i, to_t in enumerate(peers):
        remote(totals, squares.at[t], s_send.at[i], s_recv.at[t], g, to_t).start()

    @pl.loop(1, owned)
    def _(j):
        hand_out(j)

    for load in loads[1:5]:
        load.wait()

    @pl.when(g == 0)
    def _():
        loads[5].wait()
        for l in range(layers):
            @pl.loop(0, owned)
            def _(j):
                for which in range(3):
                    weights[l, j, :, which * width : (which + 1) * width] = initial[
                        l, which, j
                    ].astype(BF16)

    pick_row = lax.broadcasted_iota(jnp.int32, (16, 2 * width), 0)
    pick_lane = lax.broadcasted_iota(jnp.int32, (16, 2 * width), 1)
    spread = jnp.where(pick_row // 2 == pick_lane // width, 1.0, 0.0).astype(BF16)

    def scale_rows(l, at, sums):
        size = sums.shape[1]
        inverse = lax.rsqrt(sums / (owned * toks * width) + EPSILON)
        rate = rates[l : l + 1, at]
        inverse_high = inverse.astype(BF16).astype(F32)
        rate_high = rate.astype(BF16).astype(F32)
        at_row = lax.broadcasted_iota(jnp.int32, (16, size), 0)
        fill = jnp.where(at_row == 0, inverse_high, 0.0)
        fill = jnp.where(at_row == 1, inverse - inverse_high, fill)
        fill = jnp.where(at_row == 2, rate_high, fill)
        stack[:, at] = jnp.where(at_row == 3, rate - rate_high, fill).astype(BF16)

    def gains_of(l, j):
        rows_of = gains[:, l, lane(j, width)]
        norm = rows_of[0:1]
        return norm * rows_of[1:2], norm * rows_of[2:3], norm * rows_of[3:4], rows_of[4:5]

    def query(l, j):
        query_gain, _, _, out_gain = gains_of(l, j)
        size = min(tile, group_tok)

        @pl.loop(0, group_tok // size)
        def _(i):
            here = lane(i, size)
            stream = xin[l, j, here, :].astype(F32)
            normed = stream * dot(stack[:, here], spread[:, :width], TN)
            queries = (normed * query_gain).astype(BF16)
            both = dot(queries, weights[l, j, :, : 2 * width])
            gate = both[:, :width]
            hidden = (gate * sigmoid(gate) * both[:, width:]).astype(BF16)
            mixed = (stream + out_gain * dot(hidden, weights[l, j, :, 2 * width :])).astype(BF16)
            if l < layers - 1:
                xin[l + 1, j, here, :] = mixed
                partial[l, :, here] += sums_of(mixed)
            else:
                xout[j, here, :] = mixed

        if l == layers - 1:
            target = out.at[:, lane(t * owned + j, width)]

            @pl.when(jnp.logical_not(late))
            def _():
                for i, to_t in enumerate(peers[:far]):
                    source = xout.at[j, lane(to_t, rows)]
                    remote(source, target, o_send.at[j, i], o_recv, g, to_t).start()

            @pl.when(late)
            def _():
                for i, to_t in enumerate(peers[:far]):
                    source = xout.at[j, pl.ds(to_t * rows + kept, share)]
                    relay = g + 2 - groups
                    remote(
                        source, passing.at[j, i], q_send.at[j, i], q_recv.at[j, i], relay, t
                    ).start()
                    source = xout.at[j, pl.ds(to_t * rows, kept)]
                    remote(source, target.at[:kept], o_send.at[j, i], o_recv, g, to_t).start()

            source = xout.at[j, lane(peers[far], rows)]
            remote(source, target, o_send.at[j, far], o_recv, g, peers[far]).start()
            pltpu.make_async_copy(xout.at[j, lane(t, rows)], target, o_recv).start()

    def learn(l, j):
        _, key_gain, value_gain, _ = gains_of(l, j)
        size = min(tile, group_tok)

        def found(i):
            here = lane(i, size)
            scale = dot(stack[:, here], spread, TN)
            normed = xin[l, j, here, :].astype(F32) * scale[:, :width]
            keys = (normed * key_gain).astype(BF16)
            targets = (normed * value_gain * scale[:, width:]).astype(BF16)
            both = dot(keys, weights[l, j, :, : 2 * width])
            back = dot(targets, weights[l, j, :, 2 * width :], NT)
            gate = both[:, :width]
            up = both[:, width:]
            sig = sigmoid(gate)
            act = gate * sig
            hidden = (act * up).astype(BF16)
            back_up = (back * act).astype(BF16)
            back_gate = (back * up * (sig + act * (1.0 - sig))).astype(BF16)
            backs = jnp.concatenate([back_gate, back_up], axis=1)
            return dot(keys, backs, TN), dot(hidden, targets, TN)

        if size == group_tok:
            return found(0)
        grad_gu[...] = jnp.zeros_like(grad_gu)
        grad_d[...] = jnp.zeros_like(grad_d)

        @pl.loop(0, group_tok // size)
        def _(i):
            more_gu, more_d = found(i)
            grad_gu[...] += more_gu
            grad_d[...] += more_d

        return grad_gu[...], grad_d[...]

    def chain(l, j):
        @pl.when(g > 0)
        def _():
            arrived(weights.at[l, j], w_recv.at[l, j])

        chain_go(l, j)

    def chain_go(l, j):
        @pl.when(g < last)
        def _():
            both, below = learn(l, j)
            grads = (both[:, :width], both[:, width:], below)
            moves = tuple(
                v * lax.rsqrt(jnp.sum(v * v, axis=(0, 1), keepdims=True) + EPSILON) for v in grads
            )
            for repeat in range(NS_STEPS):
                moves = newton_schulz(moves, coarse if repeat < 2 else product)
            step = steps[l, j] * table[l, g].astype(F32)
            for which in range(3):
                at = slice(which * width, (which + 1) * width)
                entering = weights[l, j, :, at].astype(F32)
                moved = entering + step * moves[which]
                before = jnp.sum(entering * entering, axis=0, keepdims=True) + EPSILON
                after = jnp.sum(moved * moved, axis=0, keepdims=True) + EPSILON
                leaving[l, j, :, at] = (moved * (jnp.sqrt(before) * lax.rsqrt(after))).astype(BF16)
            remote(
                leaving.at[l, j], weights.at[l, j], w_send.at[l, j], w_recv.at[l, j], g + 1, t
            ).start()

    def await_tokens(j):
        for k in range(toks):
            arrived(xin.at[0, j, pl.ds(k * rows, rows)], t_recv.at[j, k])

    for to_t in peers:
        arrived(squares.at[to_t], s_recv.at[to_t])
    for k in range(toks):
        scale_rows(0, slice(k * rows, (k + 1) * rows), squares[k])

    for l in range(layers):
        if l > 0:
            arrived_sums = partial[l - 1]
            for to_t in peers:
                arrived(partials.at[l - 1, to_t], p_recv.at[l - 1, to_t])
                arrived_sums += partials[l - 1, to_t]
            scale_rows(l, slice(0, group_tok), arrived_sums)
        if l < layers - 1:
            partial[l] = jnp.zeros((1, group_tok), F32)

            @pl.loop(0, owned - 1)
            def _(j):
                if l == 0:
                    await_tokens(j)
                chain(l, j)
                query(l, j)

            if l == 0:
                await_tokens(owned - 1)

            @pl.when(g > 0)
            def _():
                arrived(weights.at[l, owned - 1], w_recv.at[l, owned - 1])

            query(l, owned - 1)
            for i, to_t in enumerate(peers):
                remote(
                    partial.at[l], partials.at[l, t], p_send.at[l, i], p_recv.at[l, t], g, to_t
                ).start()
            chain_go(l, owned - 1)
        else:
            @pl.loop(0, owned)
            def _(j):
                chain(l, j)

                @pl.when(jnp.logical_or(g == last, jnp.logical_and(g >= groups // 2, j < at_once)))
                def _():
                    query(l, j)

            @pl.when(g < last)
            def _():
                @pl.loop(jnp.where(g >= groups // 2, at_once, 0), owned)
                def _(j):
                    query(l, j)

    @pl.when(g < 2)
    def _():
        @pl.loop(0, owned)
        def _(j):
            for i, to_t in enumerate(peers[:far]):
                arrived(passing.at[j, i], q_recv.at[j, i])
                target = out.at[pl.ds(kept, share), lane(t * owned + j, width)]
                remote(
                    passing.at[j, i], target, q_send.at[j, i], o_recv, g + groups - 2, to_t
                ).start()

        @pl.loop(0, owned)
        def _(j):
            for i in range(far):
                arrived(passing.at[j, i], q_send.at[j, i])

    arrived(out, o_recv)

    @pl.loop(0, owned)
    def _(j):
        for i, to_t in enumerate(peers):
            arrived(tokens.at[:, lane(to_t * owned + j, width)], t_send.at[j, i])
        arrived(xout.at[j, :rows], o_send.at[j, far])

        @pl.when(jnp.logical_not(late))
        def _():
            for i in range(far):
                arrived(xout.at[j, :rows], o_send.at[j, i])

        @pl.when(late)
        def _():
            for i in range(far):
                arrived(xout.at[j, :kept], o_send.at[j, i])
                arrived(passing.at[j, i], q_send.at[j, i])

        @pl.when(g < last)
        def _():
            for l in range(layers):
                arrived(leaving.at[l, j], w_send.at[l, j])

    for i in range(toks - 1):
        arrived(totals, s_send.at[i])
        for l in range(layers - 1):
            arrived(partial.at[l], p_send.at[l, i])


def wave_body(tokens, learning_rates, channel_gains, fast_init, step_size, update_table):
    groups, toks = lax.axis_size("group"), lax.axis_size("tok")
    layers, _, owned, width, _ = fast_init.shape
    rows, channels = tokens.shape
    group_tok = rows * toks
    gains = channel_gains.transpose(1, 0, 2)
    sizes = (groups, toks, layers, owned, rows, width, TILE)
    anywhere = pl.BlockSpec(memory_space=pl.ANY)
    dma = pltpu.SemaphoreType.DMA
    return pl.pallas_call(
        functools.partial(wave_kernel, sizes),
        out_shape=jax.ShapeDtypeStruct((rows, channels), BF16),
        in_specs=[anywhere] * 6,
        out_specs=anywhere,
        scratch_shapes=[
            pltpu.SMEM(step_size.shape, F32),
            pltpu.SMEM(update_table.shape, jnp.int32),
            pltpu.VMEM(tokens.shape, BF16),
            pltpu.VMEM(learning_rates.shape, F32),
            pltpu.VMEM(gains.shape, F32),
            pltpu.VMEM(fast_init.shape, F32),
            pltpu.VMEM((layers, owned, group_tok, width), BF16),
            pltpu.VMEM((owned, group_tok, width), BF16),
            pltpu.VMEM((layers, owned, width, 3 * width), BF16),
            pltpu.VMEM((layers, owned, width, 3 * width), BF16),
            pltpu.VMEM((1, rows), F32),
            pltpu.VMEM((toks, 1, rows), F32),
            pltpu.VMEM((layers - 1, 1, group_tok), F32),
            pltpu.VMEM((layers - 1, toks, 1, group_tok), F32),
            pltpu.VMEM((16, group_tok), BF16),
            pltpu.VMEM((width, 2 * width), F32),
            pltpu.VMEM((width, width), F32),
            dma((owned, toks)),
            dma((owned, toks)),
            dma((toks,)),
            dma((toks,)),
            dma((layers - 1, toks)),
            dma((layers - 1, toks)),
            dma((layers, owned)),
            dma((layers, owned)),
            dma((owned, toks)),
            dma,
            dma((6,)),
            pltpu.VMEM((owned, toks - 2, rows // 256 * 80, width), BF16),
            dma((owned, toks - 2)),
            dma((owned, toks - 2)),
        ],
        compiler_params=pltpu.CompilerParams(
            collective_id=0, has_side_effects=True, vmem_limit_bytes=VMEM_LIMIT
        ),
    )(step_size, update_table, tokens, learning_rates, gains, fast_init)


TILE = 2048
VMEM_LIMIT = 67_043_328


def plan(mesh, tokens, fast_init):
    groups, toks = mesh.shape["group"], mesh.shape["tok"]
    layers, _, heads, width, _ = fast_init.shape
    rows = tokens.shape[0] // (groups * toks)
    fits = groups > 4 and toks > 2 and toks % 2 == 0 and layers > 1 and heads % toks == 0
    fits = fits and rows * toks % TILE == 0 and rows % 256 == 0 and width % 128 == 0
    return wave_body if fits and tokens.shape[0] * tokens.shape[1] <= 64 * 1024 * 1024 else body


def solution(mesh):
    in_specs = (
        P(("group", "tok"), None),
        P(None, "group"),
        P(None, None, "tok"),
        P(None, None, "tok", None, None),
        P(None, "tok"),
        P(),
    )
    out_specs = P(("group", "tok"), None)
    def run(*args):
        chosen = plan(mesh, args[0], args[3])
        return jax.shard_map(
            chosen, mesh=mesh, in_specs=in_specs, out_specs=out_specs, check_vma=False
        )(*args)

    return run
```

```python
import functools

import jax
import jax.numpy as jnp
from jax import lax
from jax.experimental import pallas as pl
from jax.experimental.pallas import tpu as pltpu
from jax.sharding import PartitionSpec as P

NS_STEPS = 5


MUON_A = 3.4445
MUON_B = -4.775
MUON_C = 2.0315
EPSILON = 1e-06


def passed_along(value, axis, by):
    size = lax.axis_size(axis)
    pairs = [(i, i + by) for i in range(size) if 0 <= i + by < size]
    return lax.ppermute(value, axis, pairs)


def orthogonalize(gradient):
    scaling = lax.rsqrt(jnp.sum(gradient * gradient, axis=(-2, -1), keepdims=True) + EPSILON)
    current = gradient * scaling
    for repeat in range(NS_STEPS):
        square = jnp.einsum("...ij,...kj->...ik", current, current, precision=lax.Precision.HIGHEST)
        polynom = MUON_B * square + MUON_C * jnp.einsum(
            "...ij,...jk->...ik", square, square, precision=lax.Precision.HIGHEST
        )
        current = MUON_A * current + jnp.einsum(
            "...ij,...jk->...ik", polynom, current, precision=lax.Precision.HIGHEST
        )
    return current


def layer_group(stream, entering, gain_rows, rates_row, steps_row, update_flag, inverse):
    row_count, channel_count = stream.shape
    heads_n = entering.shape[1]
    head_dim = entering.shape[2]
    normed = stream.astype(jnp.float32) * inverse[:, None] * gain_rows[0]
    queries = (normed * gain_rows[1]).astype(jnp.bfloat16).reshape(row_count, heads_n, head_dim)
    keys_in = (normed * gain_rows[2]).astype(jnp.bfloat16).reshape(row_count, heads_n, head_dim)
    values_in = (normed * gain_rows[3]).astype(jnp.bfloat16).reshape(row_count, heads_n, head_dim)
    rounded = entering.astype(jnp.bfloat16)
    gate_q = jnp.einsum("thi,hij->thj", queries, rounded[0], preferred_element_type=jnp.float32)
    up_q = jnp.einsum("thi,hij->thj", queries, rounded[1], preferred_element_type=jnp.float32)
    hidden_q = (jax.nn.silu(gate_q) * up_q).astype(jnp.bfloat16)
    output = jnp.einsum(
        "thj,hjk->thk", hidden_q, rounded[2], preferred_element_type=jnp.float32
    ).reshape(row_count, channel_count)
    mixed_rows = (stream.astype(jnp.float32) + gain_rows[4] * output).astype(jnp.bfloat16)
    gate_k = jnp.einsum("thi,hij->thj", keys_in, rounded[0], preferred_element_type=jnp.float32)
    up_k = jnp.einsum("thi,hij->thj", keys_in, rounded[1], preferred_element_type=jnp.float32)
    sigmoid_k = jax.nn.sigmoid(gate_k)
    active_k = gate_k * sigmoid_k
    hidden_k = (active_k * up_k).astype(jnp.bfloat16)
    targets = (rates_row[:, None, None] * values_in.astype(jnp.float32)).astype(jnp.bfloat16)
    back_hidden = jnp.einsum(
        "thk,hjk->thj", targets, rounded[2], preferred_element_type=jnp.float32
    )
    back_up = (back_hidden * active_k).astype(jnp.bfloat16)
    back_gate = (back_hidden * up_k * sigmoid_k * (1.0 + gate_k * (1.0 - sigmoid_k))).astype(
        jnp.bfloat16
    )
    grad_gate = jnp.einsum("thi,thj->hij", keys_in, back_gate, preferred_element_type=jnp.float32)
    grad_up = jnp.einsum("thi,thj->hij", keys_in, back_up, preferred_element_type=jnp.float32)
    grad_down = jnp.einsum("thj,thk->hjk", hidden_k, targets, preferred_element_type=jnp.float32)
    direction = orthogonalize(jnp.stack([grad_gate, grad_up, grad_down]))
    moved_state = entering + (update_flag * steps_row)[None, :, None, None] * direction
    norm_before = jnp.sqrt(jnp.sum(entering * entering, axis=2, keepdims=True) + EPSILON)
    norm_after = jnp.sqrt(jnp.sum(moved_state * moved_state, axis=2, keepdims=True) + EPSILON)
    return (mixed_rows, moved_state * (norm_before / norm_after))


def pass_on(outgoing):
    return passed_along(outgoing, "group", 1)


def body(tokens, learning_rates, channel_gains, fast_init, step_size, update_table):
    start_stream = lax.all_to_all(tokens, "tok", split_axis=1, concat_axis=0, tiled=True)
    group_count = lax.axis_size("group")
    group_index = lax.axis_index("group")
    width_all = start_stream.shape[1] * lax.axis_size("tok")
    layer_count = fast_init.shape[0]
    zero_state = jnp.zeros(fast_init.shape[1:], jnp.float32)

    def tick_work(stream, outgoing, layer_now, active, inverse):
        received = pass_on(outgoing)
        initial = lax.dynamic_index_in_dim(fast_init, layer_now, 0, keepdims=False)
        entering = jnp.where(group_index == 0, initial, received)
        gain_rows = lax.dynamic_index_in_dim(channel_gains, layer_now, 0, keepdims=False)
        rates_row = lax.dynamic_index_in_dim(learning_rates, layer_now, 0, keepdims=False)
        steps_row = lax.dynamic_index_in_dim(step_size, layer_now, 0, keepdims=False)
        table_cell = lax.dynamic_slice(
            update_table, (jnp.asarray(layer_now, jnp.int32), group_index), (1, 1)
        )
        update_flag = table_cell[0, 0].astype(jnp.float32)

        def working(operands):
            return layer_group(
                operands[0], operands[1], gain_rows, rates_row, steps_row, update_flag, inverse
            )

        def resting(operands):
            return (operands[0], operands[2])

        return lax.cond(active, working, resting, (stream, entering, outgoing))

    def one_tick(tick_index, loop_state):
        stream, outgoing = loop_state
        layer_raw = tick_index - group_index
        active = (layer_raw >= 0) & (layer_raw < layer_count)
        layer_now = jnp.clip(layer_raw, 0, layer_count - 1)
        widened = stream.astype(jnp.float32)
        totals = lax.psum(jnp.sum(widened * widened, axis=1), "tok")
        inverse = lax.rsqrt(totals / width_all + EPSILON)
        return tick_work(stream, outgoing, layer_now, active, inverse)

    final_stream, last_state = lax.fori_loop(
        0, layer_count + group_count - 1, one_tick, (start_stream, zero_state)
    )
    return lax.all_to_all(final_stream, "tok", split_axis=0, concat_axis=1, tiled=True)


MESH = pl.DeviceIdType.MESH
F32 = jnp.float32
BF16 = jnp.bfloat16
NN = (((1,), (0,)), ((), ()))
NT = (((1,), (1,)), ((), ()))
TN = (((0,), (0,)), ((), ()))


def dot(a, b, dims=NN):
    return lax.dot_general(a, b, dims, preferred_element_type=F32)


def halves(value):
    high = value.astype(BF16)
    return high, (value - high.astype(F32)).astype(BF16)


def product(a, b):
    a_high, a_low = halves(a)
    b_high, b_low = halves(b)
    left = jnp.concatenate([a_high, a_low], axis=1)
    above = jnp.concatenate([b_high, b_low], axis=1)
    below = jnp.concatenate([b_high, jnp.zeros_like(b_low)], axis=1)
    both = dot(left, jnp.concatenate([above, below], axis=0))
    return both[:, : b.shape[1]] + both[:, b.shape[1] :]


def sigmoid(value):
    return 0.5 * jnp.tanh(0.5 * value) + 0.5


def coarse(a, b):
    return dot(a.astype(BF16), b.astype(BF16))


def newton_schulz(values, times):
    rounded = [v.astype(BF16) for v in values]
    squares = [dot(v, v, NT) for v in rounded]
    polynoms = [MUON_B * q + MUON_C * times(q, q) for q in squares]
    return tuple(MUON_A * v + times(p, v) for p, v in zip(polynoms, values))


def wave_kernel(
    sizes,
    steps_in,
    table_in,
    tokens_in,
    rates_in,
    gains_in,
    initial_in,
    out,
    steps,
    table,
    tokens,
    rates,
    gains,
    initial,
    xin,
    xout,
    weights,
    leaving,
    totals,
    squares,
    partial,
    partials,
    scales,
    grad_gu,
    grad_d,
    t_send,
    t_recv,
    s_send,
    s_recv,
    p_send,
    p_recv,
    w_send,
    w_recv,
    o_send,
    o_recv,
    i_recv,
    passing,
    q_send,
    q_recv,
):
    groups, toks, layers, owned, rows, width, tile = sizes
    group_tok = rows * toks
    g = lax.axis_index("group")
    t = lax.axis_index("tok")
    last = groups - 1

    def remote(source, target, send, recv, to_g, to_t):
        return pltpu.make_async_remote_copy(
            src_ref=source,
            dst_ref=target,
            send_sem=send,
            recv_sem=recv,
            device_id=(to_g, to_t),
            device_id_type=MESH,
        )

    def arrived(target, recv):
        pltpu.make_async_copy(target, target, recv).wait()

    def lane(index, size):
        return pl.ds(pl.multiple_of(index * size, size), size)

    loads = [
        pltpu.make_async_copy(source, target, i_recv.at[i])
        for i, (source, target) in enumerate(
            [
                (tokens_in, tokens),
                (rates_in, rates),
                (gains_in, gains),
                (steps_in, steps),
                (table_in, table),
                (initial_in, initial),
            ]
        )
    ]
    for load in loads[:5]:
        load.start()

    @pl.when(g == 0)
    def _():
        loads[5].start()

    barrier = pltpu.get_barrier_semaphore()

    def greet(to_g, to_t):
        pl.semaphore_signal(barrier, inc=1, device_id=(to_g, to_t), device_id_type=MESH)

    chip, core = t // 2, lax.rem(t, 2)
    peers = [
        lax.rem(chip + far, toks // 2) * 2 + side for far in range(1, toks // 2) for side in range(2)
    ] + [t + 1 - 2 * core]
    for to_t in peers:
        greet(g, to_t)

    greet(lax.rem(g + 1, groups), t)
    greet(lax.rem(g + last, groups), t)
    far = toks - 2
    for away in (2, groups - 2):
        near_g = lax.rem(g + away, groups)
        greet(near_g, t)
        for to_t in peers[:far]:
            greet(near_g, to_t)
    pl.semaphore_wait(barrier, toks + 3 + 2 * far)
    share = passing.shape[2]
    kept = rows - share
    late = g >= groups - 2
    at_once = owned // 2

    def hand_out(j):
        target = xin.at[0, j, lane(t, rows)]
        for i, to_t in enumerate(peers):
            source = tokens.at[:, lane(to_t * owned + j, width)]
            remote(source, target, t_send.at[j, i], t_recv.at[j, t], g, to_t).start()
        source = tokens.at[:, lane(t * owned + j, width)]
        pltpu.make_async_copy(source, target, t_recv.at[j, t]).start()

    loads[0].wait()
    hand_out(0)
    ones_rows = jnp.ones((16, width), BF16)

    def sums_of(values):
        wide = values.astype(F32)
        return dot(ones_rows, (wide * wide).astype(BF16), NT)[0:1]

    totals[...] = jnp.zeros_like(totals)

    @pl.loop(0, owned * toks)
    def _(h):
        totals[...] += sums_of(tokens[:, lane(h, width)])

    squares[t] = totals[...]
    for i, to_t in enumerate(peers):
        remote(totals, squares.at[t], s_send.at[i], s_recv.at[t], g, to_t).start()

    @pl.loop(1, owned)
    def _(j):
        hand_out(j)

    for load in loads[1:5]:
        load.wait()

    @pl.when(g == 0)
    def _():
        loads[5].wait()
        for l in range(layers):
            @pl.loop(0, owned)
            def _(j):
                for which in range(3):
                    weights[l, j, :, which * width : (which + 1) * width] = initial[
                        l, which, j
                    ].astype(BF16)

    pick_row = lax.broadcasted_iota(jnp.int32, (16, 2 * width), 0)
    pick_lane = lax.broadcasted_iota(jnp.int32, (16, 2 * width), 1)
    spread = jnp.where(pick_row // 2 == pick_lane // width, 1.0, 0.0).astype(BF16)

    def scale_rows(l, at, sums):
        size = sums.shape[1]
        at_row = lax.broadcasted_iota(jnp.int32, (16, size), 0)
        inverse = lax.rsqrt(sums / (owned * toks * width) + EPSILON)
        rated = inverse * rates[l : l + 1, at]
        inverse_high = inverse.astype(BF16).astype(F32)
        rated_high = rated.astype(BF16).astype(F32)
        fill = jnp.where(at_row == 0, inverse_high, 0.0)
        fill = jnp.where(at_row == 1, inverse - inverse_high, fill)
        fill = jnp.where(at_row == 2, rated_high, fill)
        fill = jnp.where(at_row == 3, rated - rated_high, fill)
        scales[at, :] = dot(fill.astype(BF16), spread, TN)

    def gains_of(l, j):
        rows_of = gains[:, l, lane(j, width)]
        norm = rows_of[0:1]
        return norm * rows_of[1:2], norm * rows_of[2:3], norm * rows_of[3:4], rows_of[4:5]

    def query(l, j):
        query_gain, _, _, out_gain = gains_of(l, j)
        size = min(tile, group_tok)

        def answer(i):
            here = lane(i, size)
            stream = xin[l, j, here, :].astype(F32)
            queries = (stream * scales[here, :width] * query_gain).astype(BF16)
            both = dot(queries, weights[l, j, :, : 2 * width])
            gate = both[:, :width]
            hidden = (gate * sigmoid(gate) * both[:, width:]).astype(BF16)
            mixed = (stream + out_gain * dot(hidden, weights[l, j, :, 2 * width :])).astype(BF16)
            if l < layers - 1:
                xin[l + 1, j, here, :] = mixed
                partial[l, :, here] += sums_of(mixed)
            else:
                xout[j, here, :] = mixed

        if size == group_tok:
            answer(0)
        else:
            pl.loop(0, group_tok // size)(answer)

    def send_home(j):
        target = out.at[:, lane(t * owned + j, width)]

        @pl.when(jnp.logical_not(late))
        def _():
            for i, to_t in enumerate(peers[:far]):
                source = xout.at[j, lane(to_t, rows)]
                remote(source, target, o_send.at[j, i], o_recv, g, to_t).start()

        @pl.when(late)
        def _():
            for i, to_t in enumerate(peers[:far]):
                source = xout.at[j, pl.ds(to_t * rows + kept, share)]
                relay = g + 2 - groups
                remote(
                    source, passing.at[j, i], q_send.at[j, i], q_recv.at[j, i], relay, t
                ).start()
                source = xout.at[j, pl.ds(to_t * rows, kept)]
                remote(source, target.at[:kept], o_send.at[j, i], o_recv, g, to_t).start()

        source = xout.at[j, lane(peers[far], rows)]
        remote(source, target, o_send.at[j, far], o_recv, g, peers[far]).start()
        pltpu.make_async_copy(xout.at[j, lane(t, rows)], target, o_recv).start()

    def learn(l, j):
        _, key_gain, value_gain, _ = gains_of(l, j)
        size = min(tile, group_tok)

        def found(i):
            here = lane(i, size)
            stream = xin[l, j, here, :].astype(F32)
            keys = (stream * scales[here, :width] * key_gain).astype(BF16)
            targets = (stream * scales[here, width:] * value_gain).astype(BF16)
            both = dot(keys, weights[l, j, :, : 2 * width])
            back = dot(targets, weights[l, j, :, 2 * width :], NT)
            gate = both[:, :width]
            up = both[:, width:]
            sig = sigmoid(gate)
            act = gate * sig
            hidden = (act * up).astype(BF16)
            back_up = (back * act).astype(BF16)
            back_gate = (back * up * (sig + act * (1.0 - sig))).astype(BF16)
            backs = jnp.concatenate([back_gate, back_up], axis=1)
            return dot(keys, backs, TN), dot(hidden, targets, TN)

        if size == group_tok:
            return found(0)
        grad_gu[...] = jnp.zeros_like(grad_gu)
        grad_d[...] = jnp.zeros_like(grad_d)

        @pl.loop(0, group_tok // size)
        def _(i):
            more_gu, more_d = found(i)
            grad_gu[...] += more_gu
            grad_d[...] += more_d

        return grad_gu[...], grad_d[...]

    def chain(l, j, asked=False):
        @pl.when(g > 0)
        def _():
            arrived(weights.at[l, j], w_recv.at[l, j])

        chain_go(l, j, asked)

    def chain_go(l, j, asked=False):
        @pl.when(g < last)
        def _():
            both, below = learn(l, j)
            grads = (both[:, :width], both[:, width:], below)
            moves = tuple(
                v * lax.rsqrt(jnp.sum(v * v, axis=(0, 1), keepdims=True) + EPSILON) for v in grads
            )
            for repeat in range(NS_STEPS):
                moves = newton_schulz(moves, coarse if repeat < 2 else product)
            if asked:
                query(l, j)
            step = steps[l, j] * table[l, g].astype(F32)
            for which in range(3):
                at = slice(which * width, (which + 1) * width)
                entering = weights[l, j, :, at].astype(F32)
                moved = entering + step * moves[which]
                before = jnp.sum(entering * entering, axis=0, keepdims=True) + EPSILON
                after = jnp.sum(moved * moved, axis=0, keepdims=True) + EPSILON
                leaving[l, j, :, at] = (moved * (jnp.sqrt(before) * lax.rsqrt(after))).astype(BF16)
            remote(
                leaving.at[l, j], weights.at[l, j], w_send.at[l, j], w_recv.at[l, j], g + 1, t
            ).start()

    def await_tokens(j):
        for k in range(toks):
            arrived(xin.at[0, j, pl.ds(k * rows, rows)], t_recv.at[j, k])

    for to_t in peers:
        arrived(squares.at[to_t], s_recv.at[to_t])
    for k in range(toks):
        scale_rows(0, slice(k * rows, (k + 1) * rows), squares[k])

    for l in range(layers):
        if l > 0:
            arrived_sums = partial[l - 1]
            for to_t in peers:
                arrived(partials.at[l - 1, to_t], p_recv.at[l - 1, to_t])
                arrived_sums += partials[l - 1, to_t]
            scale_rows(l, slice(0, group_tok), arrived_sums)
        if l < layers - 1:
            partial[l] = jnp.zeros((1, group_tok), F32)

            @pl.loop(0, owned - 1)
            def _(j):
                if l == 0:
                    await_tokens(j)
                chain(l, j, True)

                @pl.when(g == last)
                def _():
                    query(l, j)

            if l == 0:
                await_tokens(owned - 1)

            @pl.when(g > 0)
            def _():
                arrived(weights.at[l, owned - 1], w_recv.at[l, owned - 1])

            query(l, owned - 1)
            for i, to_t in enumerate(peers):
                remote(
                    partial.at[l], partials.at[l, t], p_send.at[l, i], p_recv.at[l, t], g, to_t
                ).start()
            chain_go(l, owned - 1)
        else:
            @pl.loop(0, owned)
            def _(j):
                chain(l, j)

                @pl.when(jnp.logical_or(g == last, jnp.logical_and(g >= groups // 2, j < at_once)))
                def _():
                    query(l, j)
                    send_home(j)

            @pl.when(g < last)
            def _():
                @pl.loop(jnp.where(g >= groups // 2, at_once, 0), owned)
                def _(j):
                    query(l, j)
                    send_home(j)

    @pl.when(g < 2)
    def _():
        @pl.loop(0, owned)
        def _(j):
            for i, to_t in enumerate(peers[:far]):
                arrived(passing.at[j, i], q_recv.at[j, i])
                target = out.at[pl.ds(kept, share), lane(t * owned + j, width)]
                remote(
                    passing.at[j, i], target, q_send.at[j, i], o_recv, g + groups - 2, to_t
                ).start()

        @pl.loop(0, owned)
        def _(j):
            for i in range(far):
                arrived(passing.at[j, i], q_send.at[j, i])

    arrived(out, o_recv)

    @pl.loop(0, owned)
    def _(j):
        for i, to_t in enumerate(peers):
            arrived(tokens.at[:, lane(to_t * owned + j, width)], t_send.at[j, i])
        arrived(xout.at[j, :rows], o_send.at[j, far])

        @pl.when(jnp.logical_not(late))
        def _():
            for i in range(far):
                arrived(xout.at[j, :rows], o_send.at[j, i])

        @pl.when(late)
        def _():
            for i in range(far):
                arrived(xout.at[j, :kept], o_send.at[j, i])
                arrived(passing.at[j, i], q_send.at[j, i])

        @pl.when(g < last)
        def _():
            for l in range(layers):
                arrived(leaving.at[l, j], w_send.at[l, j])

    for i in range(toks - 1):
        arrived(totals, s_send.at[i])
        for l in range(layers - 1):
            arrived(partial.at[l], p_send.at[l, i])


def wave_body(tokens, learning_rates, channel_gains, fast_init, step_size, update_table):
    groups, toks = lax.axis_size("group"), lax.axis_size("tok")
    layers, _, owned, width, _ = fast_init.shape
    rows, channels = tokens.shape
    group_tok = rows * toks
    gains = channel_gains.transpose(1, 0, 2)
    sizes = (groups, toks, layers, owned, rows, width, TILE)
    anywhere = pl.BlockSpec(memory_space=pl.ANY)
    dma = pltpu.SemaphoreType.DMA
    return pl.pallas_call(
        functools.partial(wave_kernel, sizes),
        out_shape=jax.ShapeDtypeStruct((rows, channels), BF16),
        in_specs=[anywhere] * 6,
        out_specs=anywhere,
        scratch_shapes=[
            pltpu.SMEM(step_size.shape, F32),
            pltpu.SMEM(update_table.shape, jnp.int32),
            pltpu.VMEM(tokens.shape, BF16),
            pltpu.VMEM(learning_rates.shape, F32),
            pltpu.VMEM(gains.shape, F32),
            pltpu.VMEM(fast_init.shape, F32),
            pltpu.VMEM((layers, owned, group_tok, width), BF16),
            pltpu.VMEM((owned, group_tok, width), BF16),
            pltpu.VMEM((layers, owned, width, 3 * width), BF16),
            pltpu.VMEM((layers, owned, width, 3 * width), BF16),
            pltpu.VMEM((1, rows), F32),
            pltpu.VMEM((toks, 1, rows), F32),
            pltpu.VMEM((layers - 1, 1, group_tok), F32),
            pltpu.VMEM((layers - 1, toks, 1, group_tok), F32),
            pltpu.VMEM((group_tok, 2 * width), F32),
            pltpu.VMEM((width, 2 * width), F32),
            pltpu.VMEM((width, width), F32),
            dma((owned, toks)),
            dma((owned, toks)),
            dma((toks,)),
            dma((toks,)),
            dma((layers - 1, toks)),
            dma((layers - 1, toks)),
            dma((layers, owned)),
            dma((layers, owned)),
            dma((owned, toks)),
            dma,
            dma((6,)),
            pltpu.VMEM((owned, toks - 2, rows // 256 * 80, width), BF16),
            dma((owned, toks - 2)),
            dma((owned, toks - 2)),
        ],
        compiler_params=pltpu.CompilerParams(
            collective_id=0, has_side_effects=True, vmem_limit_bytes=VMEM_LIMIT
        ),
    )(step_size, update_table, tokens, learning_rates, gains, fast_init)


TILE = 2048
VMEM_LIMIT = 67_043_328


def plan(mesh, tokens, fast_init):
    groups, toks = mesh.shape["group"], mesh.shape["tok"]
    layers, _, heads, width, _ = fast_init.shape
    rows = tokens.shape[0] // (groups * toks)
    fits = groups > 4 and toks > 2 and toks % 2 == 0 and layers > 1 and heads % toks == 0
    fits = fits and rows * toks % TILE == 0 and rows % 256 == 0 and width % 128 == 0
    return wave_body if fits and tokens.shape[0] * tokens.shape[1] <= 64 * 1024 * 1024 else body


def solution(mesh):
    in_specs = (
        P(("group", "tok"), None),
        P(None, "group"),
        P(None, None, "tok"),
        P(None, None, "tok", None, None),
        P(None, "tok"),
        P(),
    )
    out_specs = P(("group", "tok"), None)
    def run(*args):
        chosen = plan(mesh, args[0], args[3])
        return jax.shard_map(
            chosen, mesh=mesh, in_specs=in_specs, out_specs=out_specs, check_vma=False
        )(*args)

    return run
```

```python
import functools

import jax
import jax.numpy as jnp
from jax import lax
from jax.experimental import pallas as pl
from jax.experimental.pallas import tpu as pltpu
from jax.sharding import PartitionSpec as P

NS_STEPS = 5


MUON_A = 3.4445
MUON_B = -4.775
MUON_C = 2.0315
EPSILON = 1e-06


def passed_along(value, axis, by):
    size = lax.axis_size(axis)
    pairs = [(i, i + by) for i in range(size) if 0 <= i + by < size]
    return lax.ppermute(value, axis, pairs)


def orthogonalize(gradient):
    scaling = lax.rsqrt(jnp.sum(gradient * gradient, axis=(-2, -1), keepdims=True) + EPSILON)
    current = gradient * scaling
    for repeat in range(NS_STEPS):
        square = jnp.einsum("...ij,...kj->...ik", current, current, precision=lax.Precision.HIGHEST)
        polynom = MUON_B * square + MUON_C * jnp.einsum(
            "...ij,...jk->...ik", square, square, precision=lax.Precision.HIGHEST
        )
        current = MUON_A * current + jnp.einsum(
            "...ij,...jk->...ik", polynom, current, precision=lax.Precision.HIGHEST
        )
    return current


def layer_group(stream, entering, gain_rows, rates_row, steps_row, update_flag, inverse):
    row_count, channel_count = stream.shape
    heads_n = entering.shape[1]
    head_dim = entering.shape[2]
    normed = stream.astype(jnp.float32) * inverse[:, None] * gain_rows[0]
    queries = (normed * gain_rows[1]).astype(jnp.bfloat16).reshape(row_count, heads_n, head_dim)
    keys_in = (normed * gain_rows[2]).astype(jnp.bfloat16).reshape(row_count, heads_n, head_dim)
    values_in = (normed * gain_rows[3]).astype(jnp.bfloat16).reshape(row_count, heads_n, head_dim)
    rounded = entering.astype(jnp.bfloat16)
    gate_q = jnp.einsum("thi,hij->thj", queries, rounded[0], preferred_element_type=jnp.float32)
    up_q = jnp.einsum("thi,hij->thj", queries, rounded[1], preferred_element_type=jnp.float32)
    hidden_q = (jax.nn.silu(gate_q) * up_q).astype(jnp.bfloat16)
    output = jnp.einsum(
        "thj,hjk->thk", hidden_q, rounded[2], preferred_element_type=jnp.float32
    ).reshape(row_count, channel_count)
    mixed_rows = (stream.astype(jnp.float32) + gain_rows[4] * output).astype(jnp.bfloat16)
    gate_k = jnp.einsum("thi,hij->thj", keys_in, rounded[0], preferred_element_type=jnp.float32)
    up_k = jnp.einsum("thi,hij->thj", keys_in, rounded[1], preferred_element_type=jnp.float32)
    sigmoid_k = jax.nn.sigmoid(gate_k)
    active_k = gate_k * sigmoid_k
    hidden_k = (active_k * up_k).astype(jnp.bfloat16)
    targets = (rates_row[:, None, None] * values_in.astype(jnp.float32)).astype(jnp.bfloat16)
    back_hidden = jnp.einsum(
        "thk,hjk->thj", targets, rounded[2], preferred_element_type=jnp.float32
    )
    back_up = (back_hidden * active_k).astype(jnp.bfloat16)
    back_gate = (back_hidden * up_k * sigmoid_k * (1.0 + gate_k * (1.0 - sigmoid_k))).astype(
        jnp.bfloat16
    )
    grad_gate = jnp.einsum("thi,thj->hij", keys_in, back_gate, preferred_element_type=jnp.float32)
    grad_up = jnp.einsum("thi,thj->hij", keys_in, back_up, preferred_element_type=jnp.float32)
    grad_down = jnp.einsum("thj,thk->hjk", hidden_k, targets, preferred_element_type=jnp.float32)
    direction = orthogonalize(jnp.stack([grad_gate, grad_up, grad_down]))
    moved_state = entering + (update_flag * steps_row)[None, :, None, None] * direction
    norm_before = jnp.sqrt(jnp.sum(entering * entering, axis=2, keepdims=True) + EPSILON)
    norm_after = jnp.sqrt(jnp.sum(moved_state * moved_state, axis=2, keepdims=True) + EPSILON)
    return (mixed_rows, moved_state * (norm_before / norm_after))


def pass_on(outgoing):
    return passed_along(outgoing, "group", 1)


def body(tokens, learning_rates, channel_gains, fast_init, step_size, update_table):
    start_stream = lax.all_to_all(tokens, "tok", split_axis=1, concat_axis=0, tiled=True)
    group_count = lax.axis_size("group")
    group_index = lax.axis_index("group")
    width_all = start_stream.shape[1] * lax.axis_size("tok")
    layer_count = fast_init.shape[0]
    zero_state = jnp.zeros(fast_init.shape[1:], jnp.float32)

    def tick_work(stream, outgoing, layer_now, active, inverse):
        received = pass_on(outgoing)
        initial = lax.dynamic_index_in_dim(fast_init, layer_now, 0, keepdims=False)
        entering = jnp.where(group_index == 0, initial, received)
        gain_rows = lax.dynamic_index_in_dim(channel_gains, layer_now, 0, keepdims=False)
        rates_row = lax.dynamic_index_in_dim(learning_rates, layer_now, 0, keepdims=False)
        steps_row = lax.dynamic_index_in_dim(step_size, layer_now, 0, keepdims=False)
        table_cell = lax.dynamic_slice(
            update_table, (jnp.asarray(layer_now, jnp.int32), group_index), (1, 1)
        )
        update_flag = table_cell[0, 0].astype(jnp.float32)

        def working(operands):
            return layer_group(
                operands[0], operands[1], gain_rows, rates_row, steps_row, update_flag, inverse
            )

        def resting(operands):
            return (operands[0], operands[2])

        return lax.cond(active, working, resting, (stream, entering, outgoing))

    def one_tick(tick_index, loop_state):
        stream, outgoing = loop_state
        layer_raw = tick_index - group_index
        active = (layer_raw >= 0) & (layer_raw < layer_count)
        layer_now = jnp.clip(layer_raw, 0, layer_count - 1)
        widened = stream.astype(jnp.float32)
        totals = lax.psum(jnp.sum(widened * widened, axis=1), "tok")
        inverse = lax.rsqrt(totals / width_all + EPSILON)
        return tick_work(stream, outgoing, layer_now, active, inverse)

    final_stream, last_state = lax.fori_loop(
        0, layer_count + group_count - 1, one_tick, (start_stream, zero_state)
    )
    return lax.all_to_all(final_stream, "tok", split_axis=0, concat_axis=1, tiled=True)


MESH = pl.DeviceIdType.MESH
F32 = jnp.float32
BF16 = jnp.bfloat16
NN = (((1,), (0,)), ((), ()))
NT = (((1,), (1,)), ((), ()))
TN = (((0,), (0,)), ((), ()))


def dot(a, b, dims=NN):
    return lax.dot_general(a, b, dims, preferred_element_type=F32)


def halves(value):
    high = value.astype(BF16)
    return high, (value - high.astype(F32)).astype(BF16)


def product(a, b):
    a_high, a_low = halves(a)
    b_high, b_low = halves(b)
    left = jnp.concatenate([a_high, a_low], axis=1)
    above = jnp.concatenate([b_high, b_low], axis=1)
    below = jnp.concatenate([b_high, jnp.zeros_like(b_low)], axis=1)
    both = dot(left, jnp.concatenate([above, below], axis=0))
    return both[:, : b.shape[1]] + both[:, b.shape[1] :]


def sigmoid(value):
    return 0.5 * jnp.tanh(0.5 * value) + 0.5


def coarse(a, b):
    return dot(a.astype(BF16), b.astype(BF16))


def newton_schulz(values, times):
    rounded = [v.astype(BF16) for v in values]
    squares = [dot(v, v, NT) for v in rounded]
    polynoms = [MUON_B * q + MUON_C * times(q, q) for q in squares]
    return tuple(MUON_A * v + times(p, v) for p, v in zip(polynoms, values))


def wave_kernel(
    sizes,
    steps_in,
    table_in,
    tokens_in,
    rates_in,
    gains_in,
    initial_in,
    out,
    steps,
    table,
    tokens,
    rates,
    gains,
    initial,
    xin,
    xout,
    weights,
    leaving,
    totals,
    squares,
    partial,
    partials,
    scales,
    grad_gu,
    grad_d,
    t_send,
    t_recv,
    s_send,
    s_recv,
    p_send,
    p_recv,
    w_send,
    w_recv,
    o_send,
    o_recv,
    i_recv,
    l_recv,
    passing,
    q_send,
    q_recv,
):
    groups, toks, layers, owned, rows, width, tile = sizes
    group_tok = rows * toks
    g = lax.axis_index("group")
    t = lax.axis_index("tok")
    last = groups - 1

    def remote(source, target, send, recv, to_g, to_t):
        return pltpu.make_async_remote_copy(
            src_ref=source,
            dst_ref=target,
            send_sem=send,
            recv_sem=recv,
            device_id=(to_g, to_t),
            device_id_type=MESH,
        )

    def arrived(target, recv):
        pltpu.make_async_copy(target, target, recv).wait()

    def lane(index, size):
        return pl.ds(pl.multiple_of(index * size, size), size)

    loads = [
        pltpu.make_async_copy(source, target, i_recv.at[i])
        for i, (source, target) in enumerate(
            [
                (rates_in, rates),
                (gains_in, gains),
                (steps_in, steps),
                (table_in, table),
                (initial_in, initial),
            ]
        )
    ]
    for load in loads[:4]:
        load.start()

    @pl.loop(0, owned)
    def _(j):
        for to_t in range(toks):
            h = to_t * owned + j
            pltpu.make_async_copy(
                tokens_in.at[:, lane(h, width)], tokens.at[h], l_recv.at[j]
            ).start()

    @pl.when(g == 0)
    def _():
        loads[4].start()

    barrier = pltpu.get_barrier_semaphore()

    def greet(to_g, to_t):
        pl.semaphore_signal(barrier, inc=1, device_id=(to_g, to_t), device_id_type=MESH)

    chip, core = t // 2, lax.rem(t, 2)
    peers = [
        lax.rem(chip + far, toks // 2) * 2 + side for far in range(1, toks // 2) for side in range(2)
    ] + [t + 1 - 2 * core]
    for to_t in peers:
        greet(g, to_t)

    greet(lax.rem(g + 1, groups), t)
    greet(lax.rem(g + last, groups), t)
    far = toks - 2
    for away in (2, groups - 2):
        near_g = lax.rem(g + away, groups)
        greet(near_g, t)
        for to_t in peers[:far]:
            greet(near_g, to_t)
    pl.semaphore_wait(barrier, toks + 3 + 2 * far)
    share = passing.shape[2]
    kept = rows - share
    late = g >= groups - 2
    at_once = owned // 2

    def hand_out(j):
        target = xin.at[0, j, lane(t, rows)]
        for i, to_t in enumerate(peers):
            source = tokens.at[to_t * owned + j]
            remote(source, target, t_send.at[j, i], t_recv.at[j, t], g, to_t).start()
        source = tokens.at[t * owned + j]
        pltpu.make_async_copy(source, target, t_recv.at[j, t]).start()

    arrived(tokens.at[:toks], l_recv.at[0])
    hand_out(0)
    ones_rows = jnp.ones((16, width), BF16)

    def sums_of(values):
        wide = values.astype(F32)
        return dot(ones_rows, (wide * wide).astype(BF16), NT)[0:1]

    for j in range(1, owned):
        arrived(tokens.at[:toks], l_recv.at[j])

    @pl.loop(0, rows // 128)
    def _(i):
        here = lane(i, 128)
        tally = jnp.zeros((128, width), F32)
        for h in range(owned * toks):
            wide = tokens[h, here, :].astype(F32)
            tally += wide * wide
        high = tally.astype(BF16)
        low = (tally - high.astype(F32)).astype(BF16)
        totals[:, here] = (dot(ones_rows, high, NT) + dot(ones_rows, low, NT))[0:1]

    squares[t] = totals[...]
    for i, to_t in enumerate(peers):
        remote(totals, squares.at[t], s_send.at[i], s_recv.at[t], g, to_t).start()

    @pl.loop(1, owned)
    def _(j):
        hand_out(j)

    for load in loads[:4]:
        load.wait()

    @pl.when(g == 0)
    def _():
        loads[4].wait()
        for l in range(layers):
            @pl.loop(0, owned)
            def _(j):
                for which in range(3):
                    weights[l, j, :, which * width : (which + 1) * width] = initial[
                        l, which, j
                    ].astype(BF16)

    pick_row = lax.broadcasted_iota(jnp.int32, (16, 2 * width), 0)
    pick_lane = lax.broadcasted_iota(jnp.int32, (16, 2 * width), 1)
    spread = jnp.where(pick_row // 2 == pick_lane // width, 1.0, 0.0).astype(BF16)

    def scale_rows(l, at, sums):
        size = sums.shape[1]
        at_row = lax.broadcasted_iota(jnp.int32, (16, size), 0)
        inverse = lax.rsqrt(sums / (owned * toks * width) + EPSILON)
        rated = inverse * rates[l : l + 1, at]
        inverse_high = inverse.astype(BF16).astype(F32)
        rated_high = rated.astype(BF16).astype(F32)
        fill = jnp.where(at_row == 0, inverse_high, 0.0)
        fill = jnp.where(at_row == 1, inverse - inverse_high, fill)
        fill = jnp.where(at_row == 2, rated_high, fill)
        fill = jnp.where(at_row == 3, rated - rated_high, fill)
        scales[at, :] = dot(fill.astype(BF16), spread, TN)

    def gains_of(l, j):
        rows_of = gains[:, l, lane(j, width)]
        norm = rows_of[0:1]
        return norm * rows_of[1:2], norm * rows_of[2:3], norm * rows_of[3:4], rows_of[4:5]

    def query(l, j):
        query_gain, _, _, out_gain = gains_of(l, j)
        size = min(tile, group_tok)

        def answer(i):
            here = lane(i, size)
            stream = xin[l, j, here, :].astype(F32)
            queries = (stream * scales[here, :width] * query_gain).astype(BF16)
            both = dot(queries, weights[l, j, :, : 2 * width])
            gate = both[:, :width]
            hidden = (gate * sigmoid(gate) * both[:, width:]).astype(BF16)
            mixed = (stream + out_gain * dot(hidden, weights[l, j, :, 2 * width :])).astype(BF16)
            if l < layers - 1:
                xin[l + 1, j, here, :] = mixed
                partial[l, :, here] += sums_of(mixed)
            else:
                xout[j, here, :] = mixed

        if size == group_tok:
            answer(0)
        else:
            pl.loop(0, group_tok // size)(answer)

    def send_home(j):
        target = out.at[:, lane(t * owned + j, width)]

        @pl.when(jnp.logical_not(late))
        def _():
            for i, to_t in enumerate(peers[:far]):
                source = xout.at[j, lane(to_t, rows)]
                remote(source, target, o_send.at[j, i], o_recv, g, to_t).start()

        @pl.when(late)
        def _():
            for i, to_t in enumerate(peers[:far]):
                source = xout.at[j, pl.ds(to_t * rows + kept, share)]
                relay = g + 2 - groups
                remote(
                    source, passing.at[j, i], q_send.at[j, i], q_recv.at[j, i], relay, t
                ).start()
                source = xout.at[j, pl.ds(to_t * rows, kept)]
                remote(source, target.at[:kept], o_send.at[j, i], o_recv, g, to_t).start()

        source = xout.at[j, lane(peers[far], rows)]
        remote(source, target, o_send.at[j, far], o_recv, g, peers[far]).start()
        pltpu.make_async_copy(xout.at[j, lane(t, rows)], target, o_recv).start()

    def learn(l, j):
        _, key_gain, value_gain, _ = gains_of(l, j)
        size = min(tile, group_tok)

        def found(i):
            here = lane(i, size)
            stream = xin[l, j, here, :].astype(F32)
            keys = (stream * scales[here, :width] * key_gain).astype(BF16)
            targets = (stream * scales[here, width:] * value_gain).astype(BF16)
            both = dot(keys, weights[l, j, :, : 2 * width])
            back = dot(targets, weights[l, j, :, 2 * width :], NT)
            gate = both[:, :width]
            up = both[:, width:]
            sig = sigmoid(gate)
            act = gate * sig
            hidden = (act * up).astype(BF16)
            back_up = (back * act).astype(BF16)
            back_gate = (back * up * (sig + act * (1.0 - sig))).astype(BF16)
            backs = jnp.concatenate([back_gate, back_up], axis=1)
            return dot(keys, backs, TN), dot(hidden, targets, TN)

        if size == group_tok:
            return found(0)
        grad_gu[...] = jnp.zeros_like(grad_gu)
        grad_d[...] = jnp.zeros_like(grad_d)

        @pl.loop(0, group_tok // size)
        def _(i):
            more_gu, more_d = found(i)
            grad_gu[...] += more_gu
            grad_d[...] += more_d

        return grad_gu[...], grad_d[...]

    def chain(l, j, asked=False):
        @pl.when(g > 0)
        def _():
            arrived(weights.at[l, j], w_recv.at[l, j])

        chain_go(l, j, asked)

    def chain_go(l, j, asked=False):
        @pl.when(g < last)
        def _():
            both, below = learn(l, j)
            grads = (both[:, :width], both[:, width:], below)
            moves = tuple(
                v * lax.rsqrt(jnp.sum(v * v, axis=(0, 1), keepdims=True) + EPSILON) for v in grads
            )
            for repeat in range(NS_STEPS):
                moves = newton_schulz(moves, coarse if repeat < 2 else product)
            if asked:
                query(l, j)
            step = steps[l, j] * table[l, g].astype(F32)
            for which in range(3):
                at = slice(which * width, (which + 1) * width)
                entering = weights[l, j, :, at].astype(F32)
                moved = entering + step * moves[which]
                before = jnp.sum(entering * entering, axis=0, keepdims=True) + EPSILON
                after = jnp.sum(moved * moved, axis=0, keepdims=True) + EPSILON
                leaving[l, j, :, at] = (moved * (jnp.sqrt(before) * lax.rsqrt(after))).astype(BF16)
            remote(
                leaving.at[l, j], weights.at[l, j], w_send.at[l, j], w_recv.at[l, j], g + 1, t
            ).start()

    def await_tokens(j):
        for k in range(toks):
            arrived(xin.at[0, j, pl.ds(k * rows, rows)], t_recv.at[j, k])

    for to_t in peers:
        arrived(squares.at[to_t], s_recv.at[to_t])
    for k in range(toks):
        scale_rows(0, slice(k * rows, (k + 1) * rows), squares[k])

    for l in range(layers):
        if l > 0:
            arrived_sums = partial[l - 1]
            for to_t in peers:
                arrived(partials.at[l - 1, to_t], p_recv.at[l - 1, to_t])
                arrived_sums += partials[l - 1, to_t]
            scale_rows(l, slice(0, group_tok), arrived_sums)
        if l < layers - 1:
            partial[l] = jnp.zeros((1, group_tok), F32)

            @pl.loop(0, owned - 1)
            def _(j):
                if l == 0:
                    await_tokens(j)
                chain(l, j, True)

                @pl.when(g == last)
                def _():
                    query(l, j)

            if l == 0:
                await_tokens(owned - 1)

            @pl.when(g > 0)
            def _():
                arrived(weights.at[l, owned - 1], w_recv.at[l, owned - 1])

            query(l, owned - 1)
            for i, to_t in enumerate(peers):
                remote(
                    partial.at[l], partials.at[l, t], p_send.at[l, i], p_recv.at[l, t], g, to_t
                ).start()
            chain_go(l, owned - 1)
        else:
            @pl.loop(0, owned)
            def _(j):
                chain(l, j)

                @pl.when(jnp.logical_or(g == last, jnp.logical_and(g >= groups // 2, j < at_once)))
                def _():
                    query(l, j)
                    send_home(j)

            @pl.when(g < last)
            def _():
                @pl.loop(jnp.where(g >= groups // 2, at_once, 0), owned)
                def _(j):
                    query(l, j)
                    send_home(j)

    @pl.when(g < 2)
    def _():
        @pl.loop(0, owned)
        def _(j):
            for i, to_t in enumerate(peers[:far]):
                arrived(passing.at[j, i], q_recv.at[j, i])
                target = out.at[pl.ds(kept, share), lane(t * owned + j, width)]
                remote(
                    passing.at[j, i], target, q_send.at[j, i], o_recv, g + groups - 2, to_t
                ).start()

        @pl.loop(0, owned)
        def _(j):
            for i in range(far):
                arrived(passing.at[j, i], q_send.at[j, i])

    arrived(out, o_recv)

    @pl.loop(0, owned)
    def _(j):
        for i, to_t in enumerate(peers):
            arrived(tokens.at[to_t * owned + j], t_send.at[j, i])
        arrived(xout.at[j, :rows], o_send.at[j, far])

        @pl.when(jnp.logical_not(late))
        def _():
            for i in range(far):
                arrived(xout.at[j, :rows], o_send.at[j, i])

        @pl.when(late)
        def _():
            for i in range(far):
                arrived(xout.at[j, :kept], o_send.at[j, i])
                arrived(passing.at[j, i], q_send.at[j, i])

        @pl.when(g < last)
        def _():
            for l in range(layers):
                arrived(leaving.at[l, j], w_send.at[l, j])

    for i in range(toks - 1):
        arrived(totals, s_send.at[i])
        for l in range(layers - 1):
            arrived(partial.at[l], p_send.at[l, i])


def wave_body(tokens, learning_rates, channel_gains, fast_init, step_size, update_table):
    groups, toks = lax.axis_size("group"), lax.axis_size("tok")
    layers, _, owned, width, _ = fast_init.shape
    rows, channels = tokens.shape
    group_tok = rows * toks
    gains = channel_gains.transpose(1, 0, 2)
    sizes = (groups, toks, layers, owned, rows, width, TILE)
    pin = lambda x: pltpu.with_memory_space_constraint(x, pltpu.HBM)
    anywhere = pl.BlockSpec(memory_space=pl.ANY)
    dma = pltpu.SemaphoreType.DMA
    return pl.pallas_call(
        functools.partial(wave_kernel, sizes),
        out_shape=jax.ShapeDtypeStruct((rows, channels), BF16),
        in_specs=[anywhere] * 6,
        out_specs=anywhere,
        scratch_shapes=[
            pltpu.SMEM(step_size.shape, F32),
            pltpu.SMEM(update_table.shape, jnp.int32),
            pltpu.VMEM((channels // width, rows, width), BF16),
            pltpu.VMEM(learning_rates.shape, F32),
            pltpu.VMEM(gains.shape, F32),
            pltpu.VMEM(fast_init.shape, F32),
            pltpu.VMEM((layers, owned, group_tok, width), BF16),
            pltpu.VMEM((owned, group_tok, width), BF16),
            pltpu.VMEM((layers, owned, width, 3 * width), BF16),
            pltpu.VMEM((layers, owned, width, 3 * width), BF16),
            pltpu.VMEM((1, rows), F32),
            pltpu.VMEM((toks, 1, rows), F32),
            pltpu.VMEM((layers - 1, 1, group_tok), F32),
            pltpu.VMEM((layers - 1, toks, 1, group_tok), F32),
            pltpu.VMEM((group_tok, 2 * width), F32),
            pltpu.VMEM((width, 2 * width), F32),
            pltpu.VMEM((width, width), F32),
            dma((owned, toks)),
            dma((owned, toks)),
            dma((toks,)),
            dma((toks,)),
            dma((layers - 1, toks)),
            dma((layers - 1, toks)),
            dma((layers, owned)),
            dma((layers, owned)),
            dma((owned, toks)),
            dma,
            dma((5,)),
            dma((owned,)),
            pltpu.VMEM((owned, toks - 2, rows // 256 * 80, width), BF16),
            dma((owned, toks - 2)),
            dma((owned, toks - 2)),
        ],
        compiler_params=pltpu.CompilerParams(
            collective_id=0, has_side_effects=True, vmem_limit_bytes=VMEM_LIMIT
        ),
    )(*map(pin, (step_size, update_table, tokens, learning_rates, gains, fast_init)))


TILE = 2048
VMEM_LIMIT = 50 * 1024 * 1024


def plan(mesh, tokens, fast_init):
    groups, toks = mesh.shape["group"], mesh.shape["tok"]
    layers, _, heads, width, _ = fast_init.shape
    rows = tokens.shape[0] // (groups * toks)
    fits = groups > 4 and toks > 2 and toks % 2 == 0 and layers > 1 and heads % toks == 0
    fits = fits and rows * toks % TILE == 0 and rows % 256 == 0 and width % 128 == 0
    return wave_body if fits and tokens.shape[0] * tokens.shape[1] <= 64 * 1024 * 1024 else body


def solution(mesh):
    in_specs = (
        P(("group", "tok"), None),
        P(None, "group"),
        P(None, None, "tok"),
        P(None, None, "tok", None, None),
        P(None, "tok"),
        P(),
    )
    out_specs = P(("group", "tok"), None)
    def run(*args):
        chosen = plan(mesh, args[0], args[3])
        return jax.shard_map(
            chosen, mesh=mesh, in_specs=in_specs, out_specs=out_specs, check_vma=False
        )(*args)

    return run
```

```python
import functools

import jax
import jax.numpy as jnp
from jax import lax
from jax.experimental import pallas as pl
from jax.experimental.pallas import tpu as pltpu
from jax.sharding import PartitionSpec as P

NS_STEPS = 5


MUON_A = 3.4445
MUON_B = -4.775
MUON_C = 2.0315
EPSILON = 1e-06


def passed_along(value, axis, by):
    size = lax.axis_size(axis)
    pairs = [(i, i + by) for i in range(size) if 0 <= i + by < size]
    return lax.ppermute(value, axis, pairs)


def orthogonalize(gradient):
    scaling = lax.rsqrt(jnp.sum(gradient * gradient, axis=(-2, -1), keepdims=True) + EPSILON)
    current = gradient * scaling
    for repeat in range(NS_STEPS):
        square = jnp.einsum("...ij,...kj->...ik", current, current, precision=lax.Precision.HIGHEST)
        polynom = MUON_B * square + MUON_C * jnp.einsum(
            "...ij,...jk->...ik", square, square, precision=lax.Precision.HIGHEST
        )
        current = MUON_A * current + jnp.einsum(
            "...ij,...jk->...ik", polynom, current, precision=lax.Precision.HIGHEST
        )
    return current


def layer_group(stream, entering, gain_rows, rates_row, steps_row, update_flag, inverse):
    row_count, channel_count = stream.shape
    heads_n = entering.shape[1]
    head_dim = entering.shape[2]
    normed = stream.astype(jnp.float32) * inverse[:, None] * gain_rows[0]
    queries = (normed * gain_rows[1]).astype(jnp.bfloat16).reshape(row_count, heads_n, head_dim)
    keys_in = (normed * gain_rows[2]).astype(jnp.bfloat16).reshape(row_count, heads_n, head_dim)
    values_in = (normed * gain_rows[3]).astype(jnp.bfloat16).reshape(row_count, heads_n, head_dim)
    rounded = entering.astype(jnp.bfloat16)
    gate_q = jnp.einsum("thi,hij->thj", queries, rounded[0], preferred_element_type=jnp.float32)
    up_q = jnp.einsum("thi,hij->thj", queries, rounded[1], preferred_element_type=jnp.float32)
    hidden_q = (jax.nn.silu(gate_q) * up_q).astype(jnp.bfloat16)
    output = jnp.einsum(
        "thj,hjk->thk", hidden_q, rounded[2], preferred_element_type=jnp.float32
    ).reshape(row_count, channel_count)
    mixed_rows = (stream.astype(jnp.float32) + gain_rows[4] * output).astype(jnp.bfloat16)
    gate_k = jnp.einsum("thi,hij->thj", keys_in, rounded[0], preferred_element_type=jnp.float32)
    up_k = jnp.einsum("thi,hij->thj", keys_in, rounded[1], preferred_element_type=jnp.float32)
    sigmoid_k = jax.nn.sigmoid(gate_k)
    active_k = gate_k * sigmoid_k
    hidden_k = (active_k * up_k).astype(jnp.bfloat16)
    targets = (rates_row[:, None, None] * values_in.astype(jnp.float32)).astype(jnp.bfloat16)
    back_hidden = jnp.einsum(
        "thk,hjk->thj", targets, rounded[2], preferred_element_type=jnp.float32
    )
    back_up = (back_hidden * active_k).astype(jnp.bfloat16)
    back_gate = (back_hidden * up_k * sigmoid_k * (1.0 + gate_k * (1.0 - sigmoid_k))).astype(
        jnp.bfloat16
    )
    grad_gate = jnp.einsum("thi,thj->hij", keys_in, back_gate, preferred_element_type=jnp.float32)
    grad_up = jnp.einsum("thi,thj->hij", keys_in, back_up, preferred_element_type=jnp.float32)
    grad_down = jnp.einsum("thj,thk->hjk", hidden_k, targets, preferred_element_type=jnp.float32)
    direction = orthogonalize(jnp.stack([grad_gate, grad_up, grad_down]))
    moved_state = entering + (update_flag * steps_row)[None, :, None, None] * direction
    norm_before = jnp.sqrt(jnp.sum(entering * entering, axis=2, keepdims=True) + EPSILON)
    norm_after = jnp.sqrt(jnp.sum(moved_state * moved_state, axis=2, keepdims=True) + EPSILON)
    return (mixed_rows, moved_state * (norm_before / norm_after))


def pass_on(outgoing):
    return passed_along(outgoing, "group", 1)


def body(tokens, learning_rates, channel_gains, fast_init, step_size, update_table):
    start_stream = lax.all_to_all(tokens, "tok", split_axis=1, concat_axis=0, tiled=True)
    group_count = lax.axis_size("group")
    group_index = lax.axis_index("group")
    width_all = start_stream.shape[1] * lax.axis_size("tok")
    layer_count = fast_init.shape[0]
    zero_state = jnp.zeros(fast_init.shape[1:], jnp.float32)

    def tick_work(stream, outgoing, layer_now, active, inverse):
        received = pass_on(outgoing)
        initial = lax.dynamic_index_in_dim(fast_init, layer_now, 0, keepdims=False)
        entering = jnp.where(group_index == 0, initial, received)
        gain_rows = lax.dynamic_index_in_dim(channel_gains, layer_now, 0, keepdims=False)
        rates_row = lax.dynamic_index_in_dim(learning_rates, layer_now, 0, keepdims=False)
        steps_row = lax.dynamic_index_in_dim(step_size, layer_now, 0, keepdims=False)
        table_cell = lax.dynamic_slice(
            update_table, (jnp.asarray(layer_now, jnp.int32), group_index), (1, 1)
        )
        update_flag = table_cell[0, 0].astype(jnp.float32)

        def working(operands):
            return layer_group(
                operands[0], operands[1], gain_rows, rates_row, steps_row, update_flag, inverse
            )

        def resting(operands):
            return (operands[0], operands[2])

        return lax.cond(active, working, resting, (stream, entering, outgoing))

    def one_tick(tick_index, loop_state):
        stream, outgoing = loop_state
        layer_raw = tick_index - group_index
        active = (layer_raw >= 0) & (layer_raw < layer_count)
        layer_now = jnp.clip(layer_raw, 0, layer_count - 1)
        widened = stream.astype(jnp.float32)
        totals = lax.psum(jnp.sum(widened * widened, axis=1), "tok")
        inverse = lax.rsqrt(totals / width_all + EPSILON)
        return tick_work(stream, outgoing, layer_now, active, inverse)

    final_stream, last_state = lax.fori_loop(
        0, layer_count + group_count - 1, one_tick, (start_stream, zero_state)
    )
    return lax.all_to_all(final_stream, "tok", split_axis=0, concat_axis=1, tiled=True)


MESH = pl.DeviceIdType.MESH
F32 = jnp.float32
BF16 = jnp.bfloat16
NN = (((1,), (0,)), ((), ()))
NT = (((1,), (1,)), ((), ()))
TN = (((0,), (0,)), ((), ()))


def dot(a, b, dims=NN):
    return lax.dot_general(a, b, dims, preferred_element_type=F32)


def halves(value):
    high = value.astype(BF16)
    return high, (value - high.astype(F32)).astype(BF16)


def product(a, b):
    a_high, a_low = halves(a)
    b_high, b_low = halves(b)
    left = jnp.concatenate([a_high, a_low], axis=1)
    above = jnp.concatenate([b_high, b_low], axis=1)
    below = jnp.concatenate([b_high, jnp.zeros_like(b_low)], axis=1)
    both = dot(left, jnp.concatenate([above, below], axis=0))
    return both[:, : b.shape[1]] + both[:, b.shape[1] :]


def sigmoid(value):
    return 0.5 * jnp.tanh(0.5 * value) + 0.5


def coarse(a, b):
    return dot(a.astype(BF16), b.astype(BF16))


def first_step(values):
    rounded = [v.astype(BF16) for v in values]
    squares = [dot(v, v, NT) for v in rounded]
    scales = [
        lax.rsqrt(jnp.sum(v * v, axis=(0, 1), keepdims=True) + EPSILON) for v in values
    ]
    squares = [q * (r * r) for q, r in zip(squares, scales)]
    polynoms = [MUON_B * q + MUON_C * coarse(q, q) for q in squares]
    return tuple(
        r * (MUON_A * v + dot(p.astype(BF16), n))
        for p, v, n, r in zip(polynoms, values, rounded, scales)
    )


def newton_schulz(values, times):
    rounded = [v.astype(BF16) for v in values]
    squares = [dot(v, v, NT) for v in rounded]
    polynoms = [MUON_B * q + MUON_C * times(q, q) for q in squares]
    return tuple(MUON_A * v + times(p, v) for p, v in zip(polynoms, values))


def wave_kernel(
    sizes,
    steps_in,
    table_in,
    tokens_in,
    rates_in,
    gains_in,
    initial_in,
    out,
    steps,
    table,
    tokens,
    rates,
    gains,
    initial,
    xin,
    xout,
    weights,
    leaving,
    totals,
    squares,
    partial,
    partials,
    scales,
    grad_gu,
    grad_d,
    t_send,
    t_recv,
    s_send,
    s_recv,
    p_send,
    p_recv,
    w_send,
    w_recv,
    o_send,
    o_recv,
    i_recv,
    l_recv,
    passing,
    q_send,
    q_recv,
):
    groups, toks, layers, owned, rows, width, tile = sizes
    group_tok = rows * toks
    g = lax.axis_index("group")
    t = lax.axis_index("tok")
    last = groups - 1

    def remote(source, target, send, recv, to_g, to_t):
        return pltpu.make_async_remote_copy(
            src_ref=source,
            dst_ref=target,
            send_sem=send,
            recv_sem=recv,
            device_id=(to_g, to_t),
            device_id_type=MESH,
        )

    def arrived(target, recv):
        pltpu.make_async_copy(target, target, recv).wait()

    def lane(index, size):
        return pl.ds(pl.multiple_of(index * size, size), size)

    loads = [
        pltpu.make_async_copy(source, target, i_recv.at[i])
        for i, (source, target) in enumerate(
            [
                (rates_in, rates),
                (gains_in, gains),
                (steps_in, steps),
                (table_in, table),
                (initial_in, initial),
            ]
        )
    ]
    barrier = pltpu.get_barrier_semaphore()

    def greet(to_g, to_t):
        pl.semaphore_signal(barrier, inc=1, device_id=(to_g, to_t), device_id_type=MESH)

    chip, core = t // 2, lax.rem(t, 2)
    peers = [
        lax.rem(chip + far, toks // 2) * 2 + side for far in range(1, toks // 2) for side in range(2)
    ] + [t + 1 - 2 * core]
    for to_t in peers:
        greet(g, to_t)

    greet(lax.rem(g + 1, groups), t)
    greet(lax.rem(g + last, groups), t)
    far = toks - 2
    for away in (2, groups - 2):
        near_g = lax.rem(g + away, groups)
        greet(near_g, t)
        for to_t in peers[:far]:
            greet(near_g, to_t)
    for load in loads[:4]:
        load.start()

    @pl.loop(0, owned)
    def _(j):
        for to_t in range(toks):
            h = to_t * owned + j
            pltpu.make_async_copy(
                tokens_in.at[:, lane(h, width)], tokens.at[h], l_recv.at[j]
            ).start()

    @pl.when(g == 0)
    def _():
        loads[4].start()

    pl.semaphore_wait(barrier, toks + 3 + 2 * far)
    share = passing.shape[2]
    kept = rows - share
    late = g >= groups - 2
    at_once = owned // 2

    def hand_out(j):
        target = xin.at[0, j, lane(t, rows)]
        for i, to_t in enumerate(peers):
            source = tokens.at[to_t * owned + j]
            remote(source, target, t_send.at[j, i], t_recv.at[j, t], g, to_t).start()
        source = tokens.at[t * owned + j]
        pltpu.make_async_copy(source, target, t_recv.at[j, t]).start()

    arrived(tokens.at[:toks], l_recv.at[0])
    hand_out(0)
    ones_rows = jnp.ones((16, width), BF16)

    def sums_of(values):
        wide = values.astype(F32)
        return dot(ones_rows, (wide * wide).astype(BF16), NT)[0:1]

    for j in range(1, owned):
        arrived(tokens.at[:toks], l_recv.at[j])

    @pl.loop(0, rows // 128)
    def _(i):
        here = lane(i, 128)
        tally = jnp.zeros((128, width), F32)
        for h in range(owned * toks):
            wide = tokens[h, here, :].astype(F32)
            tally += wide * wide
        high = tally.astype(BF16)
        low = (tally - high.astype(F32)).astype(BF16)
        totals[:, here] = (dot(ones_rows, high, NT) + dot(ones_rows, low, NT))[0:1]

    squares[t] = totals[...]
    for i, to_t in enumerate(peers):
        remote(totals, squares.at[t], s_send.at[i], s_recv.at[t], g, to_t).start()

    @pl.loop(1, owned)
    def _(j):
        hand_out(j)

    for load in loads[:4]:
        load.wait()

    @pl.when(g == 0)
    def _():
        loads[4].wait()
        for l in range(layers):
            @pl.loop(0, owned)
            def _(j):
                for which in range(3):
                    weights[l, j, :, which * width : (which + 1) * width] = initial[
                        l, which, j
                    ].astype(BF16)

    pick_row = lax.broadcasted_iota(jnp.int32, (16, 2 * width), 0)
    pick_lane = lax.broadcasted_iota(jnp.int32, (16, 2 * width), 1)
    spread = jnp.where(pick_row // 2 == pick_lane // width, 1.0, 0.0).astype(BF16)

    def scale_rows(l, at, sums):
        size = sums.shape[1]
        at_row = lax.broadcasted_iota(jnp.int32, (16, size), 0)
        inverse = lax.rsqrt(sums / (owned * toks * width) + EPSILON)
        rated = inverse * rates[l : l + 1, at]
        inverse_high = inverse.astype(BF16).astype(F32)
        rated_high = rated.astype(BF16).astype(F32)
        fill = jnp.where(at_row == 0, inverse_high, 0.0)
        fill = jnp.where(at_row == 1, inverse - inverse_high, fill)
        fill = jnp.where(at_row == 2, rated_high, fill)
        fill = jnp.where(at_row == 3, rated - rated_high, fill)
        scales[at, :] = dot(fill.astype(BF16), spread, TN)

    def gains_of(l, j):
        rows_of = gains[:, l, lane(j, width)]
        norm = rows_of[0:1]
        return norm * rows_of[1:2], norm * rows_of[2:3], norm * rows_of[3:4], rows_of[4:5]

    def query(l, j):
        query_gain, _, _, out_gain = gains_of(l, j)
        size = min(tile, group_tok)

        def answer(i):
            here = lane(i, size)
            stream = xin[l, j, here, :].astype(F32)
            queries = (stream * scales[here, :width] * query_gain).astype(BF16)
            both = dot(queries, weights[l, j, :, : 2 * width])
            gate = both[:, :width]
            hidden = (gate * sigmoid(gate) * both[:, width:]).astype(BF16)
            mixed = (stream + out_gain * dot(hidden, weights[l, j, :, 2 * width :])).astype(BF16)
            if l < layers - 1:
                xin[l + 1, j, here, :] = mixed
                partial[l, :, here] += sums_of(mixed)
            else:
                xout[j, here, :] = mixed

        if size == group_tok:
            answer(0)
        else:
            pl.loop(0, group_tok // size)(answer)

    def send_home(j):
        target = out.at[:, lane(t * owned + j, width)]

        @pl.when(jnp.logical_not(late))
        def _():
            for i, to_t in enumerate(peers[:far]):
                source = xout.at[j, lane(to_t, rows)]
                remote(source, target, o_send.at[j, i], o_recv, g, to_t).start()

        @pl.when(late)
        def _():
            for i, to_t in enumerate(peers[:far]):
                source = xout.at[j, pl.ds(to_t * rows + kept, share)]
                relay = g + 2 - groups
                remote(
                    source, passing.at[j, i], q_send.at[j, i], q_recv.at[j, i], relay, t
                ).start()
                source = xout.at[j, pl.ds(to_t * rows, kept)]
                remote(source, target.at[:kept], o_send.at[j, i], o_recv, g, to_t).start()

        source = xout.at[j, lane(peers[far], rows)]
        remote(source, target, o_send.at[j, far], o_recv, g, peers[far]).start()
        pltpu.make_async_copy(xout.at[j, lane(t, rows)], target, o_recv).start()

    def learn(l, j):
        _, key_gain, value_gain, _ = gains_of(l, j)
        size = min(tile, group_tok)

        def found(i):
            here = lane(i, size)
            stream = xin[l, j, here, :].astype(F32)
            keys = (stream * scales[here, :width] * key_gain).astype(BF16)
            targets = (stream * scales[here, width:] * value_gain).astype(BF16)
            both = dot(keys, weights[l, j, :, : 2 * width])
            back = dot(targets, weights[l, j, :, 2 * width :], NT)
            gate = both[:, :width]
            up = both[:, width:]
            sig = sigmoid(gate)
            act = gate * sig
            hidden = (act * up).astype(BF16)
            back_up = (back * act).astype(BF16)
            back_gate = (back * up * (sig + act * (1.0 - sig))).astype(BF16)
            backs = jnp.concatenate([back_gate, back_up], axis=1)
            return dot(keys, backs, TN), dot(hidden, targets, TN)

        if size == group_tok:
            return found(0)
        grad_gu[...] = jnp.zeros_like(grad_gu)
        grad_d[...] = jnp.zeros_like(grad_d)

        @pl.loop(0, group_tok // size)
        def _(i):
            more_gu, more_d = found(i)
            grad_gu[...] += more_gu
            grad_d[...] += more_d

        return grad_gu[...], grad_d[...]

    def chain(l, j, asked=False):
        @pl.when(g > 0)
        def _():
            arrived(weights.at[l, j], w_recv.at[l, j])

        chain_go(l, j, asked)

    def chain_go(l, j, asked=False):
        @pl.when(g < last)
        def _():
            both, below = learn(l, j)
            grads = (both[:, :width], both[:, width:], below)
            moves = first_step(grads)
            for repeat in range(1, NS_STEPS):
                moves = newton_schulz(moves, coarse if repeat < 2 else product)
            if asked:
                query(l, j)
            step = steps[l, j] * table[l, g].astype(F32)
            for which in range(3):
                at = slice(which * width, (which + 1) * width)
                entering = weights[l, j, :, at].astype(F32)
                moved = entering + step * moves[which]
                before = jnp.sum(entering * entering, axis=0, keepdims=True) + EPSILON
                after = jnp.sum(moved * moved, axis=0, keepdims=True) + EPSILON
                leaving[l, j, :, at] = (moved * (jnp.sqrt(before) * lax.rsqrt(after))).astype(BF16)
            remote(
                leaving.at[l, j], weights.at[l, j], w_send.at[l, j], w_recv.at[l, j], g + 1, t
            ).start()

    def await_tokens(j):
        for k in range(toks):
            arrived(xin.at[0, j, pl.ds(k * rows, rows)], t_recv.at[j, k])

    for to_t in peers:
        arrived(squares.at[to_t], s_recv.at[to_t])
    for k in range(toks):
        scale_rows(0, slice(k * rows, (k + 1) * rows), squares[k])

    for l in range(layers):
        if l > 0:
            arrived_sums = partial[l - 1]
            for to_t in peers:
                arrived(partials.at[l - 1, to_t], p_recv.at[l - 1, to_t])
                arrived_sums += partials[l - 1, to_t]
            scale_rows(l, slice(0, group_tok), arrived_sums)
        if l < layers - 1:
            partial[l] = jnp.zeros((1, group_tok), F32)

            @pl.loop(0, owned - 1)
            def _(j):
                if l == 0:
                    await_tokens(j)
                chain(l, j, True)

                @pl.when(g == last)
                def _():
                    query(l, j)

            if l == 0:
                await_tokens(owned - 1)

            @pl.when(g > 0)
            def _():
                arrived(weights.at[l, owned - 1], w_recv.at[l, owned - 1])

            query(l, owned - 1)
            for i, to_t in enumerate(peers):
                remote(
                    partial.at[l], partials.at[l, t], p_send.at[l, i], p_recv.at[l, t], g, to_t
                ).start()
            chain_go(l, owned - 1)
        else:
            @pl.loop(0, owned)
            def _(j):
                chain(l, j)

                @pl.when(jnp.logical_or(g == last, jnp.logical_and(g >= groups // 2, j < at_once)))
                def _():
                    query(l, j)
                    send_home(j)

            @pl.when(g < last)
            def _():
                @pl.loop(jnp.where(g >= groups // 2, at_once, 0), owned)
                def _(j):
                    query(l, j)
                    send_home(j)

    @pl.when(g < 2)
    def _():
        @pl.loop(0, owned)
        def _(j):
            for i, to_t in enumerate(peers[:far]):
                arrived(passing.at[j, i], q_recv.at[j, i])
                target = out.at[pl.ds(kept, share), lane(t * owned + j, width)]
                remote(
                    passing.at[j, i], target, q_send.at[j, i], o_recv, g + groups - 2, to_t
                ).start()

        @pl.loop(0, owned)
        def _(j):
            for i in range(far):
                arrived(passing.at[j, i], q_send.at[j, i])

    arrived(out, o_recv)

    @pl.loop(0, owned)
    def _(j):
        for i, to_t in enumerate(peers):
            arrived(tokens.at[to_t * owned + j], t_send.at[j, i])
        arrived(xout.at[j, :rows], o_send.at[j, far])

        @pl.when(jnp.logical_not(late))
        def _():
            for i in range(far):
                arrived(xout.at[j, :rows], o_send.at[j, i])

        @pl.when(late)
        def _():
            for i in range(far):
                arrived(xout.at[j, :kept], o_send.at[j, i])
                arrived(passing.at[j, i], q_send.at[j, i])

        @pl.when(g < last)
        def _():
            for l in range(layers):
                arrived(leaving.at[l, j], w_send.at[l, j])

    for i in range(toks - 1):
        arrived(totals, s_send.at[i])
        for l in range(layers - 1):
            arrived(partial.at[l], p_send.at[l, i])


def wave_body(tokens, learning_rates, channel_gains, fast_init, step_size, update_table):
    groups, toks = lax.axis_size("group"), lax.axis_size("tok")
    layers, _, owned, width, _ = fast_init.shape
    rows, channels = tokens.shape
    group_tok = rows * toks
    gains = channel_gains.transpose(1, 0, 2)
    sizes = (groups, toks, layers, owned, rows, width, TILE)
    pin = lambda x: pltpu.with_memory_space_constraint(x, pltpu.HBM)
    anywhere = pl.BlockSpec(memory_space=pl.ANY)
    dma = pltpu.SemaphoreType.DMA
    return pl.pallas_call(
        functools.partial(wave_kernel, sizes),
        out_shape=jax.ShapeDtypeStruct((rows, channels), BF16),
        in_specs=[anywhere] * 6,
        out_specs=anywhere,
        scratch_shapes=[
            pltpu.SMEM(step_size.shape, F32),
            pltpu.SMEM(update_table.shape, jnp.int32),
            pltpu.VMEM((channels // width, rows, width), BF16),
            pltpu.VMEM(learning_rates.shape, F32),
            pltpu.VMEM(gains.shape, F32),
            pltpu.VMEM(fast_init.shape, F32),
            pltpu.VMEM((layers, owned, group_tok, width), BF16),
            pltpu.VMEM((owned, group_tok, width), BF16),
            pltpu.VMEM((layers, owned, width, 3 * width), BF16),
            pltpu.VMEM((layers, owned, width, 3 * width), BF16),
            pltpu.VMEM((1, rows), F32),
            pltpu.VMEM((toks, 1, rows), F32),
            pltpu.VMEM((layers - 1, 1, group_tok), F32),
            pltpu.VMEM((layers - 1, toks, 1, group_tok), F32),
            pltpu.VMEM((group_tok, 2 * width), F32),
            pltpu.VMEM((width, 2 * width), F32),
            pltpu.VMEM((width, width), F32),
            dma((owned, toks)),
            dma((owned, toks)),
            dma((toks,)),
            dma((toks,)),
            dma((layers - 1, toks)),
            dma((layers - 1, toks)),
            dma((layers, owned)),
            dma((layers, owned)),
            dma((owned, toks)),
            dma,
            dma((5,)),
            dma((owned,)),
            pltpu.VMEM((owned, toks - 2, rows // 256 * 80, width), BF16),
            dma((owned, toks - 2)),
            dma((owned, toks - 2)),
        ],
        compiler_params=pltpu.CompilerParams(
            collective_id=0, has_side_effects=True, vmem_limit_bytes=VMEM_LIMIT
        ),
    )(*map(pin, (step_size, update_table, tokens, learning_rates, gains, fast_init)))


TILE = 2048
VMEM_LIMIT = 50 * 1024 * 1024


def plan(mesh, tokens, fast_init):
    groups, toks = mesh.shape["group"], mesh.shape["tok"]
    layers, _, heads, width, _ = fast_init.shape
    rows = tokens.shape[0] // (groups * toks)
    fits = groups > 4 and toks > 2 and toks % 2 == 0 and layers > 1 and heads % toks == 0
    fits = fits and rows * toks % TILE == 0 and rows % 256 == 0 and width % 128 == 0
    return wave_body if fits and tokens.shape[0] * tokens.shape[1] <= 64 * 1024 * 1024 else body


def solution(mesh):
    in_specs = (
        P(("group", "tok"), None),
        P(None, "group"),
        P(None, None, "tok"),
        P(None, None, "tok", None, None),
        P(None, "tok"),
        P(),
    )
    out_specs = P(("group", "tok"), None)
    def run(*args):
        chosen = plan(mesh, args[0], args[3])
        return jax.shard_map(
            chosen, mesh=mesh, in_specs=in_specs, out_specs=out_specs, check_vma=False
        )(*args)

    return run
```

```python
import functools

import jax
import jax.numpy as jnp
from jax import lax
from jax.experimental import pallas as pl
from jax.experimental.pallas import tpu as pltpu
from jax.sharding import PartitionSpec as P

NS_STEPS = 5


MUON_A = 3.4445
MUON_B = -4.775
MUON_C = 2.0315
EPSILON = 1e-06


def passed_along(value, axis, by):
    size = lax.axis_size(axis)
    pairs = [(i, i + by) for i in range(size) if 0 <= i + by < size]
    return lax.ppermute(value, axis, pairs)


def orthogonalize(gradient):
    scaling = lax.rsqrt(jnp.sum(gradient * gradient, axis=(-2, -1), keepdims=True) + EPSILON)
    current = gradient * scaling
    for repeat in range(NS_STEPS):
        square = jnp.einsum("...ij,...kj->...ik", current, current, precision=lax.Precision.HIGHEST)
        polynom = MUON_B * square + MUON_C * jnp.einsum(
            "...ij,...jk->...ik", square, square, precision=lax.Precision.HIGHEST
        )
        current = MUON_A * current + jnp.einsum(
            "...ij,...jk->...ik", polynom, current, precision=lax.Precision.HIGHEST
        )
    return current


def layer_group(stream, entering, gain_rows, rates_row, steps_row, update_flag, inverse):
    row_count, channel_count = stream.shape
    heads_n = entering.shape[1]
    head_dim = entering.shape[2]
    normed = stream.astype(jnp.float32) * inverse[:, None] * gain_rows[0]
    queries = (normed * gain_rows[1]).astype(jnp.bfloat16).reshape(row_count, heads_n, head_dim)
    keys_in = (normed * gain_rows[2]).astype(jnp.bfloat16).reshape(row_count, heads_n, head_dim)
    values_in = (normed * gain_rows[3]).astype(jnp.bfloat16).reshape(row_count, heads_n, head_dim)
    rounded = entering.astype(jnp.bfloat16)
    gate_q = jnp.einsum("thi,hij->thj", queries, rounded[0], preferred_element_type=jnp.float32)
    up_q = jnp.einsum("thi,hij->thj", queries, rounded[1], preferred_element_type=jnp.float32)
    hidden_q = (jax.nn.silu(gate_q) * up_q).astype(jnp.bfloat16)
    output = jnp.einsum(
        "thj,hjk->thk", hidden_q, rounded[2], preferred_element_type=jnp.float32
    ).reshape(row_count, channel_count)
    mixed_rows = (stream.astype(jnp.float32) + gain_rows[4] * output).astype(jnp.bfloat16)
    gate_k = jnp.einsum("thi,hij->thj", keys_in, rounded[0], preferred_element_type=jnp.float32)
    up_k = jnp.einsum("thi,hij->thj", keys_in, rounded[1], preferred_element_type=jnp.float32)
    sigmoid_k = jax.nn.sigmoid(gate_k)
    active_k = gate_k * sigmoid_k
    hidden_k = (active_k * up_k).astype(jnp.bfloat16)
    targets = (rates_row[:, None, None] * values_in.astype(jnp.float32)).astype(jnp.bfloat16)
    back_hidden = jnp.einsum(
        "thk,hjk->thj", targets, rounded[2], preferred_element_type=jnp.float32
    )
    back_up = (back_hidden * active_k).astype(jnp.bfloat16)
    back_gate = (back_hidden * up_k * sigmoid_k * (1.0 + gate_k * (1.0 - sigmoid_k))).astype(
        jnp.bfloat16
    )
    grad_gate = jnp.einsum("thi,thj->hij", keys_in, back_gate, preferred_element_type=jnp.float32)
    grad_up = jnp.einsum("thi,thj->hij", keys_in, back_up, preferred_element_type=jnp.float32)
    grad_down = jnp.einsum("thj,thk->hjk", hidden_k, targets, preferred_element_type=jnp.float32)
    direction = orthogonalize(jnp.stack([grad_gate, grad_up, grad_down]))
    moved_state = entering + (update_flag * steps_row)[None, :, None, None] * direction
    norm_before = jnp.sqrt(jnp.sum(entering * entering, axis=2, keepdims=True) + EPSILON)
    norm_after = jnp.sqrt(jnp.sum(moved_state * moved_state, axis=2, keepdims=True) + EPSILON)
    return (mixed_rows, moved_state * (norm_before / norm_after))


def pass_on(outgoing):
    return passed_along(outgoing, "group", 1)


def body(tokens, learning_rates, channel_gains, fast_init, step_size, update_table):
    start_stream = lax.all_to_all(tokens, "tok", split_axis=1, concat_axis=0, tiled=True)
    group_count = lax.axis_size("group")
    group_index = lax.axis_index("group")
    width_all = start_stream.shape[1] * lax.axis_size("tok")
    layer_count = fast_init.shape[0]
    zero_state = jnp.zeros(fast_init.shape[1:], jnp.float32)

    def tick_work(stream, outgoing, layer_now, active, inverse):
        received = pass_on(outgoing)
        initial = lax.dynamic_index_in_dim(fast_init, layer_now, 0, keepdims=False)
        entering = jnp.where(group_index == 0, initial, received)
        gain_rows = lax.dynamic_index_in_dim(channel_gains, layer_now, 0, keepdims=False)
        rates_row = lax.dynamic_index_in_dim(learning_rates, layer_now, 0, keepdims=False)
        steps_row = lax.dynamic_index_in_dim(step_size, layer_now, 0, keepdims=False)
        table_cell = lax.dynamic_slice(
            update_table, (jnp.asarray(layer_now, jnp.int32), group_index), (1, 1)
        )
        update_flag = table_cell[0, 0].astype(jnp.float32)

        def working(operands):
            return layer_group(
                operands[0], operands[1], gain_rows, rates_row, steps_row, update_flag, inverse
            )

        def resting(operands):
            return (operands[0], operands[2])

        return lax.cond(active, working, resting, (stream, entering, outgoing))

    def one_tick(tick_index, loop_state):
        stream, outgoing = loop_state
        layer_raw = tick_index - group_index
        active = (layer_raw >= 0) & (layer_raw < layer_count)
        layer_now = jnp.clip(layer_raw, 0, layer_count - 1)
        widened = stream.astype(jnp.float32)
        totals = lax.psum(jnp.sum(widened * widened, axis=1), "tok")
        inverse = lax.rsqrt(totals / width_all + EPSILON)
        return tick_work(stream, outgoing, layer_now, active, inverse)

    final_stream, last_state = lax.fori_loop(
        0, layer_count + group_count - 1, one_tick, (start_stream, zero_state)
    )
    return lax.all_to_all(final_stream, "tok", split_axis=0, concat_axis=1, tiled=True)


MESH = pl.DeviceIdType.MESH
F32 = jnp.float32
BF16 = jnp.bfloat16
NN = (((1,), (0,)), ((), ()))
NT = (((1,), (1,)), ((), ()))
TN = (((0,), (0,)), ((), ()))


def dot(a, b, dims=NN):
    return lax.dot_general(a, b, dims, preferred_element_type=F32)


def halves(value):
    high = value.astype(BF16)
    return high, (value - high.astype(F32)).astype(BF16)


def product(a, b):
    a_high, a_low = halves(a)
    b_high, b_low = halves(b)
    left = jnp.concatenate([a_high, a_low], axis=1)
    above = jnp.concatenate([b_high, b_low], axis=1)
    below = jnp.concatenate([b_high, jnp.zeros_like(b_low)], axis=1)
    both = dot(left, jnp.concatenate([above, below], axis=0))
    return both[:, : b.shape[1]] + both[:, b.shape[1] :]


def sigmoid(value):
    return 0.5 * jnp.tanh(0.5 * value) + 0.5


def coarse(a, b):
    return dot(a.astype(BF16), b.astype(BF16))


def first_step(values):
    rounded = [v.astype(BF16) for v in values]
    squares = [dot(v, v, NT) for v in rounded]
    scales = [
        lax.rsqrt(jnp.sum(v * v, axis=(0, 1), keepdims=True) + EPSILON) for v in values
    ]
    squares = [q * (r * r) for q, r in zip(squares, scales)]
    polynoms = [MUON_B * q + MUON_C * coarse(q, q) for q in squares]
    return tuple(
        r * (MUON_A * v + dot(p.astype(BF16), n))
        for p, v, n, r in zip(polynoms, values, rounded, scales)
    )


def newton_schulz(values, times):
    rounded = [v.astype(BF16) for v in values]
    squares = [dot(v, v, NT) for v in rounded]
    polynoms = [MUON_B * q + MUON_C * times(q, q) for q in squares]
    return tuple(MUON_A * v + times(p, v) for p, v in zip(polynoms, values))


def wave_kernel(
    sizes,
    steps_in,
    table_in,
    tokens_in,
    rates_in,
    gains_in,
    initial_in,
    out,
    steps,
    table,
    tokens,
    rates,
    gains,
    initial,
    xin,
    xout,
    weights,
    leaving,
    totals,
    squares,
    partial,
    partials,
    scales,
    grad_gu,
    grad_d,
    t_send,
    t_recv,
    s_send,
    s_recv,
    p_send,
    p_recv,
    w_send,
    w_recv,
    o_send,
    o_recv,
    i_recv,
    l_recv,
    passing,
    q_send,
    q_recv,
):
    groups, toks, layers, owned, rows, width, tile = sizes
    group_tok = rows * toks
    g = lax.axis_index("group")
    t = lax.axis_index("tok")
    last = groups - 1

    def remote(source, target, send, recv, to_g, to_t):
        return pltpu.make_async_remote_copy(
            src_ref=source,
            dst_ref=target,
            send_sem=send,
            recv_sem=recv,
            device_id=(to_g, to_t),
            device_id_type=MESH,
        )

    def arrived(target, recv):
        pltpu.make_async_copy(target, target, recv).wait()

    def lane(index, size):
        return pl.ds(pl.multiple_of(index * size, size), size)

    loads = [
        pltpu.make_async_copy(source, target, i_recv.at[i])
        for i, (source, target) in enumerate(
            [
                (rates_in, rates),
                (gains_in, gains),
                (steps_in, steps),
                (table_in, table),
                (initial_in, initial),
            ]
        )
    ]
    barrier = pltpu.get_barrier_semaphore()

    def greet(to_g, to_t):
        pl.semaphore_signal(barrier, inc=1, device_id=(to_g, to_t), device_id_type=MESH)

    chip, core = t // 2, lax.rem(t, 2)
    peers = [
        lax.rem(chip + far, toks // 2) * 2 + side for far in range(1, toks // 2) for side in range(2)
    ] + [t + 1 - 2 * core]
    for to_t in peers:
        greet(g, to_t)

    greet(lax.rem(g + 1, groups), t)
    greet(lax.rem(g + last, groups), t)
    far = toks - 2
    for away in (2, groups - 2):
        near_g = lax.rem(g + away, groups)
        greet(near_g, t)
        for to_t in peers[:far]:
            greet(near_g, to_t)
    for load in loads[:4]:
        load.start()

    @pl.loop(0, owned)
    def _(j):
        for to_t in range(toks):
            h = to_t * owned + j
            pltpu.make_async_copy(
                tokens_in.at[:, lane(h, width)], tokens.at[h], l_recv.at[j]
            ).start()

    @pl.when(g == 0)
    def _():
        loads[4].start()

    pl.semaphore_wait(barrier, toks + 3 + 2 * far)
    share = passing.shape[2]
    kept = rows - share
    late = g >= groups - 2
    at_once = owned // 2

    def hand_out(j):
        target = xin.at[0, j, lane(t, rows)]
        for i, to_t in enumerate(peers):
            source = tokens.at[to_t * owned + j]
            remote(source, target, t_send.at[j, i], t_recv.at[j, t], g, to_t).start()
        source = tokens.at[t * owned + j]
        pltpu.make_async_copy(source, target, t_recv.at[j, t]).start()

    arrived(tokens.at[:toks], l_recv.at[0])
    hand_out(0)
    ones_rows = jnp.ones((16, width), BF16)

    def sums_of(values):
        wide = values.astype(F32)
        return dot(ones_rows, (wide * wide).astype(BF16), NT)[0:1]

    for j in range(1, owned):
        arrived(tokens.at[:toks], l_recv.at[j])

    @pl.loop(0, rows // 128)
    def _(i):
        here = lane(i, 128)
        tally = jnp.zeros((128, width), F32)
        for h in range(owned * toks):
            wide = tokens[h, here, :].astype(F32)
            tally += wide * wide
        high = tally.astype(BF16)
        low = (tally - high.astype(F32)).astype(BF16)
        totals[:, here] = (dot(ones_rows, high, NT) + dot(ones_rows, low, NT))[0:1]

    squares[t] = totals[...]
    for i, to_t in enumerate(peers):
        remote(totals, squares.at[t], s_send.at[i], s_recv.at[t], g, to_t).start()

    @pl.loop(1, owned)
    def _(j):
        hand_out(j)

    for load in loads[:4]:
        load.wait()

    @pl.when(g == 0)
    def _():
        loads[4].wait()
        for l in range(layers):
            @pl.loop(0, owned)
            def _(j):
                for which in range(3):
                    weights[l, j, :, which * width : (which + 1) * width] = initial[
                        l, which, j
                    ].astype(BF16)

    pick_row = lax.broadcasted_iota(jnp.int32, (16, 2 * width), 0)
    pick_lane = lax.broadcasted_iota(jnp.int32, (16, 2 * width), 1)
    spread = jnp.where(pick_row // 2 == pick_lane // width, 1.0, 0.0).astype(BF16)

    def scale_rows(l, at, sums):
        size = sums.shape[1]
        at_row = lax.broadcasted_iota(jnp.int32, (16, size), 0)
        inverse = lax.rsqrt(sums / (owned * toks * width) + EPSILON)
        rated = inverse * rates[l : l + 1, at]
        inverse_high = inverse.astype(BF16).astype(F32)
        rated_high = rated.astype(BF16).astype(F32)
        fill = jnp.where(at_row == 0, inverse_high, 0.0)
        fill = jnp.where(at_row == 1, inverse - inverse_high, fill)
        fill = jnp.where(at_row == 2, rated_high, fill)
        fill = jnp.where(at_row == 3, rated - rated_high, fill)
        scales[at, :] = dot(fill.astype(BF16), spread, TN)

    def gains_of(l, j):
        rows_of = gains[:, l, lane(j, width)]
        norm = rows_of[0:1]
        return norm * rows_of[1:2], norm * rows_of[2:3], norm * rows_of[3:4], rows_of[4:5]

    def query(l, j):
        query_gain, _, _, out_gain = gains_of(l, j)
        size = min(tile, group_tok)

        def answer(i):
            here = lane(i, size)
            stream = xin[l, j, here, :].astype(F32)
            queries = (stream * scales[here, :width] * query_gain).astype(BF16)
            both = dot(queries, weights[l, j, :, : 2 * width])
            gate = both[:, :width]
            hidden = (gate * sigmoid(gate) * both[:, width:]).astype(BF16)
            mixed = (stream + out_gain * dot(hidden, weights[l, j, :, 2 * width :])).astype(BF16)
            if l < layers - 1:
                xin[l + 1, j, here, :] = mixed
                partial[l, :, here] += sums_of(mixed)
            else:
                xout[j, here, :] = mixed

        if size == group_tok:
            answer(0)
        else:
            pl.loop(0, group_tok // size)(answer)

    def send_home(j):
        target = out.at[:, lane(t * owned + j, width)]

        @pl.when(jnp.logical_not(late))
        def _():
            for i, to_t in enumerate(peers[:far]):
                source = xout.at[j, lane(to_t, rows)]
                remote(source, target, o_send.at[j, i], o_recv, g, to_t).start()

        @pl.when(late)
        def _():
            for i, to_t in enumerate(peers[:far]):
                source = xout.at[j, pl.ds(to_t * rows + kept, share)]
                relay = g + 2 - groups
                remote(
                    source, passing.at[j, i], q_send.at[j, i], q_recv.at[j, i], relay, t
                ).start()
                source = xout.at[j, pl.ds(to_t * rows, kept)]
                remote(source, target.at[:kept], o_send.at[j, i], o_recv, g, to_t).start()

        source = xout.at[j, lane(peers[far], rows)]
        remote(source, target, o_send.at[j, far], o_recv, g, peers[far]).start()
        pltpu.make_async_copy(xout.at[j, lane(t, rows)], target, o_recv).start()

    def learn(l, j):
        _, key_gain, value_gain, _ = gains_of(l, j)
        size = min(tile, group_tok)

        def found(i):
            here = lane(i, size)
            stream = xin[l, j, here, :].astype(F32)
            keys = (stream * scales[here, :width] * key_gain).astype(BF16)
            targets = (stream * scales[here, width:] * value_gain).astype(BF16)
            both = dot(keys, weights[l, j, :, : 2 * width])
            back = dot(targets, weights[l, j, :, 2 * width :], NT)
            gate = both[:, :width]
            up = both[:, width:]
            sig = sigmoid(gate)
            act = gate * sig
            hidden = (act * up).astype(BF16)
            back_up = (back * act).astype(BF16)
            back_gate = (back * up * (sig + act * (1.0 - sig))).astype(BF16)
            backs = jnp.concatenate([back_gate, back_up], axis=1)
            return dot(keys, backs, TN), dot(hidden, targets, TN)

        if size == group_tok:
            return found(0)
        grad_gu[...] = jnp.zeros_like(grad_gu)
        grad_d[...] = jnp.zeros_like(grad_d)

        @pl.loop(0, group_tok // size)
        def _(i):
            more_gu, more_d = found(i)
            grad_gu[...] += more_gu
            grad_d[...] += more_d

        return grad_gu[...], grad_d[...]

    def chain(l, j, asked=False):
        @pl.when(g > 0)
        def _():
            arrived(weights.at[l, j], w_recv.at[l, j])

        chain_go(l, j, asked)

    def chain_go(l, j, asked=False):
        @pl.when(g < last)
        def _():
            both, below = learn(l, j)
            grads = (both[:, :width], both[:, width:], below)
            moves = first_step(grads)
            for repeat in range(1, NS_STEPS):
                moves = newton_schulz(moves, coarse if repeat < 2 else product)
            if asked:
                query(l, j)
            step = steps[l, j] * table[l, g].astype(F32)
            for which in range(3):
                at = slice(which * width, (which + 1) * width)
                entering = weights[l, j, :, at].astype(F32)
                moved = entering + step * moves[which]
                before = jnp.sum(entering * entering, axis=0, keepdims=True) + EPSILON
                after = jnp.sum(moved * moved, axis=0, keepdims=True) + EPSILON
                leaving[l, j, :, at] = (moved * (jnp.sqrt(before) * lax.rsqrt(after))).astype(BF16)
            remote(
                leaving.at[l, j], weights.at[l, j], w_send.at[l, j], w_recv.at[l, j], g + 1, t
            ).start()

    def await_tokens(j):
        for k in range(toks):
            arrived(xin.at[0, j, pl.ds(k * rows, rows)], t_recv.at[j, k])

    for to_t in peers:
        arrived(squares.at[to_t], s_recv.at[to_t])
    for k in range(toks):
        scale_rows(0, slice(k * rows, (k + 1) * rows), squares[k])

    for l in range(layers):
        if l > 0:
            arrived_sums = partial[l - 1]
            for to_t in peers:
                arrived(partials.at[l - 1, to_t], p_recv.at[l - 1, to_t])
                arrived_sums += partials[l - 1, to_t]
            scale_rows(l, slice(0, group_tok), arrived_sums)
        if l < layers - 1:
            partial[l] = jnp.zeros((1, group_tok), F32)

            @pl.loop(0, owned - 1)
            def _(j):
                if l == 0:
                    await_tokens(j)
                chain(l, j, True)

                @pl.when(g == last)
                def _():
                    query(l, j)

            if l == 0:
                await_tokens(owned - 1)

            @pl.when(g > 0)
            def _():
                arrived(weights.at[l, owned - 1], w_recv.at[l, owned - 1])

            query(l, owned - 1)
            for i, to_t in enumerate(peers):
                remote(
                    partial.at[l], partials.at[l, t], p_send.at[l, i], p_recv.at[l, t], g, to_t
                ).start()
            chain_go(l, owned - 1)
        else:
            @pl.loop(0, owned)
            def _(j):
                here = jnp.logical_and(g >= groups // 2, jnp.logical_or(g == last, j < at_once))

                @pl.when(here)
                def _():
                    chain(l, j, True)

                    @pl.when(g == last)
                    def _():
                        query(l, j)

                    send_home(j)

                @pl.when(jnp.logical_not(here))
                def _():
                    chain(l, j)

            @pl.when(g < last)
            def _():
                @pl.loop(jnp.where(g >= groups // 2, at_once, 0), owned)
                def _(j):
                    query(l, j)
                    send_home(j)

    @pl.when(g < 2)
    def _():
        @pl.loop(0, owned)
        def _(j):
            for i, to_t in enumerate(peers[:far]):
                arrived(passing.at[j, i], q_recv.at[j, i])
                target = out.at[pl.ds(kept, share), lane(t * owned + j, width)]
                remote(
                    passing.at[j, i], target, q_send.at[j, i], o_recv, g + groups - 2, to_t
                ).start()

        @pl.loop(0, owned)
        def _(j):
            for i in range(far):
                arrived(passing.at[j, i], q_send.at[j, i])

    arrived(out, o_recv)

    @pl.loop(0, owned)
    def _(j):
        for i, to_t in enumerate(peers):
            arrived(tokens.at[to_t * owned + j], t_send.at[j, i])
        arrived(xout.at[j, :rows], o_send.at[j, far])

        @pl.when(jnp.logical_not(late))
        def _():
            for i in range(far):
                arrived(xout.at[j, :rows], o_send.at[j, i])

        @pl.when(late)
        def _():
            for i in range(far):
                arrived(xout.at[j, :kept], o_send.at[j, i])
                arrived(passing.at[j, i], q_send.at[j, i])

        @pl.when(g < last)
        def _():
            for l in range(layers):
                arrived(leaving.at[l, j], w_send.at[l, j])

    for i in range(toks - 1):
        arrived(totals, s_send.at[i])
        for l in range(layers - 1):
            arrived(partial.at[l], p_send.at[l, i])


def wave_body(tokens, learning_rates, channel_gains, fast_init, step_size, update_table):
    groups, toks = lax.axis_size("group"), lax.axis_size("tok")
    layers, _, owned, width, _ = fast_init.shape
    rows, channels = tokens.shape
    group_tok = rows * toks
    gains = channel_gains.transpose(1, 0, 2)
    sizes = (groups, toks, layers, owned, rows, width, TILE)
    pin = lambda x: pltpu.with_memory_space_constraint(x, pltpu.HBM)
    anywhere = pl.BlockSpec(memory_space=pl.ANY)
    dma = pltpu.SemaphoreType.DMA
    return pl.pallas_call(
        functools.partial(wave_kernel, sizes),
        out_shape=jax.ShapeDtypeStruct((rows, channels), BF16),
        in_specs=[anywhere] * 6,
        out_specs=anywhere,
        scratch_shapes=[
            pltpu.SMEM(step_size.shape, F32),
            pltpu.SMEM(update_table.shape, jnp.int32),
            pltpu.VMEM((channels // width, rows, width), BF16),
            pltpu.VMEM(learning_rates.shape, F32),
            pltpu.VMEM(gains.shape, F32),
            pltpu.VMEM(fast_init.shape, F32),
            pltpu.VMEM((layers, owned, group_tok, width), BF16),
            pltpu.VMEM((owned, group_tok, width), BF16),
            pltpu.VMEM((layers, owned, width, 3 * width), BF16),
            pltpu.VMEM((layers, owned, width, 3 * width), BF16),
            pltpu.VMEM((1, rows), F32),
            pltpu.VMEM((toks, 1, rows), F32),
            pltpu.VMEM((layers - 1, 1, group_tok), F32),
            pltpu.VMEM((layers - 1, toks, 1, group_tok), F32),
            pltpu.VMEM((group_tok, 2 * width), F32),
            pltpu.VMEM((width, 2 * width), F32),
            pltpu.VMEM((width, width), F32),
            dma((owned, toks)),
            dma((owned, toks)),
            dma((toks,)),
            dma((toks,)),
            dma((layers - 1, toks)),
            dma((layers - 1, toks)),
            dma((layers, owned)),
            dma((layers, owned)),
            dma((owned, toks)),
            dma,
            dma((5,)),
            dma((owned,)),
            pltpu.VMEM((owned, toks - 2, rows // 256 * 80, width), BF16),
            dma((owned, toks - 2)),
            dma((owned, toks - 2)),
        ],
        compiler_params=pltpu.CompilerParams(
            collective_id=0, has_side_effects=True, vmem_limit_bytes=VMEM_LIMIT
        ),
    )(*map(pin, (step_size, update_table, tokens, learning_rates, gains, fast_init)))


TILE = 2048
VMEM_LIMIT = 50 * 1024 * 1024


def plan(mesh, tokens, fast_init):
    groups, toks = mesh.shape["group"], mesh.shape["tok"]
    layers, _, heads, width, _ = fast_init.shape
    rows = tokens.shape[0] // (groups * toks)
    fits = groups > 4 and toks > 2 and toks % 2 == 0 and layers > 1 and heads % toks == 0
    fits = fits and rows * toks % TILE == 0 and rows % 256 == 0 and width % 128 == 0
    return wave_body if fits and tokens.shape[0] * tokens.shape[1] <= 64 * 1024 * 1024 else body


def solution(mesh):
    in_specs = (
        P(("group", "tok"), None),
        P(None, "group"),
        P(None, None, "tok"),
        P(None, None, "tok", None, None),
        P(None, "tok"),
        P(),
    )
    out_specs = P(("group", "tok"), None)
    def run(*args):
        chosen = plan(mesh, args[0], args[3])
        return jax.shard_map(
            chosen, mesh=mesh, in_specs=in_specs, out_specs=out_specs, check_vma=False
        )(*args)

    return run
```
